8 devices in a mesh: problem: 1 (over z), samp: 2 (over y), feat: 4 (over x, core).
Axes of the slice: x: 2, y: 2, z: 1, core: 2. Of those that a mesh axis runs over, the one named last changes fastest.
Arguments:
- design: bfloat16 [16384, 16384], P(('problem', 'samp'), 'feat')
- targets: float32 [16384, 256], P(('problem', 'samp'))
- coef_init: float32 [16384, 256], P(('problem', 'feat'))
- step_sizes: float32 [16384], P(('problem', 'feat'))
- ridge_weights: float32 [256], P('problem')
Outputs:
- output 1: float32 [16384, 256], P(('problem', 'feat'))
- output 2: float32 [16384, 256], P(('problem', 'samp'))
All inputs are finite; a program needn't handle non-finite values.
Results may differ from the reference program's by a relative error of at most 0.00678921.
Values are sent between devices in bfloat16 or wider.
A program may use at most 1 GiB of HBM per device.

```python
import jax
import jax.numpy as jnp
from jax import lax

NUM_ROWS = 16384
NUM_FEATURES = 16384
NUM_TARGETS = 256
FEAT_BLOCKS = 4
SWEEPS = 4
STEP_WEIGHT = 0.5


def setup_inputs(seed: int = 0, part: int = 0) -> dict:
    base_key = jax.random.fold_in(jax.random.key(seed), part)
    sub_keys = jax.random.split(base_key, 9)
    shared_rank = 8
    shared_mix = 0.8
    row_block = NUM_ROWS // 8
    factors = jax.random.normal(sub_keys[0], (NUM_ROWS, shared_rank), jnp.float32)
    loadings = jax.random.normal(sub_keys[1], (shared_rank, NUM_FEATURES), jnp.float32)

    def draw_rows(block_index):
        rows_f = lax.dynamic_slice_in_dim(factors, block_index * row_block, row_block, 0)
        shared = jnp.dot(rows_f, loadings) * (shared_mix / shared_rank) ** 0.5
        noise_blk = jax.random.normal(jax.random.fold_in(sub_keys[2], block_index), (row_block, NUM_FEATURES), jnp.float32)
        return (shared + (1.0 - shared_mix) ** 0.5 * noise_blk).astype(jnp.bfloat16)

    design = lax.map(draw_rows, jnp.arange(8)).reshape(NUM_ROWS, NUM_FEATURES)

    def power_step(step_index, probe_vec):
        unit_vec = probe_vec / jnp.linalg.norm(probe_vec)
        image_vec = jnp.dot(design, unit_vec.astype(jnp.bfloat16), preferred_element_type=jnp.float32)
        return jnp.dot(image_vec.astype(jnp.bfloat16), design, preferred_element_type=jnp.float32) / NUM_ROWS

    probe_init = jax.random.normal(sub_keys[3], (NUM_FEATURES,), jnp.float32)
    curvature = 1.15 * jnp.linalg.norm(lax.fori_loop(0, 12, power_step, probe_init))
    step_sizes = jax.random.uniform(sub_keys[4], (NUM_FEATURES,), jnp.float32, 0.4, 0.8) / curvature
    ridge_weights = jax.random.uniform(sub_keys[5], (NUM_TARGETS,), jnp.float32, 0.05, 0.25) * curvature
    coef_init = jax.random.normal(sub_keys[6], (NUM_FEATURES, NUM_TARGETS), jnp.float32) * NUM_FEATURES ** -0.5
    w_star = jax.random.normal(sub_keys[7], (NUM_FEATURES, NUM_TARGETS), jnp.float32) * NUM_FEATURES ** -0.5
    targets = jnp.dot(design, w_star.astype(jnp.bfloat16), preferred_element_type=jnp.float32) + 0.3 * jax.random.normal(sub_keys[8], (NUM_ROWS, NUM_TARGETS), jnp.float32)
    return {"design": design, "targets": targets, "coef_init": coef_init, "step_sizes": step_sizes, "ridge_weights": ridge_weights}


def reference(design, targets, coef_init, step_sizes, ridge_weights):
    block_cols = NUM_FEATURES // FEAT_BLOCKS

    def block_sum(weights):
        weights_b = weights.astype(jnp.bfloat16)

        def add_block(acc_sum, block_index):
            col_block = lax.dynamic_slice_in_dim(design, block_index * block_cols, block_cols, 1)
            rows_w = lax.dynamic_slice_in_dim(weights_b, block_index * block_cols, block_cols, 0)
            product = jnp.dot(col_block, rows_w, preferred_element_type=jnp.float32)
            return acc_sum + product.astype(jnp.bfloat16).astype(jnp.float32), None

        return lax.scan(add_block, jnp.zeros((NUM_ROWS, NUM_TARGETS), jnp.float32), jnp.arange(FEAT_BLOCKS))[0]

    def sweep_once(sweep_state, unused):
        coef_cur, resid_cur = sweep_state
        gradient = lax.dot_general(design, resid_cur.astype(jnp.bfloat16), (((0,), (0,)), ((), ())), preferred_element_type=jnp.float32) / NUM_ROWS
        step_delta = step_sizes[:, None] * (gradient - ridge_weights[None, :] * coef_cur)
        return (coef_cur + STEP_WEIGHT * step_delta, resid_cur - STEP_WEIGHT * block_sum(step_delta)), None

    start_state = (coef_init, targets - block_sum(coef_init))
    final_state = lax.scan(sweep_once, start_state, None, length=SWEEPS)[0]
    return final_state[0], final_state[1]
```

```python
import functools

import jax
import jax.numpy as jnp
from jax import lax
from jax.experimental import pallas as pl
from jax.experimental.pallas import tpu as pltpu
from jax.sharding import PartitionSpec as P

SWEEPS = 4
STEP_WEIGHT = 0.5
MESH = pl.DeviceIdType.MESH

RING = 8
LAG_SUM = 2
LAG_RELAY = 4
LAG_GRAD = 4
EXTRA = 2
FIRST_CHUNK = 3
GROUPS = 2


def kernel(x_hbm, y_hbm, w0_hbm, w0b_hbm, eta_hbm, lam_hbm, w_out, r_out,
           xb, sb, gb, gr, wb, eb, lb, rb, rt, ub, ur, fr,
           x_sem, in_sem, us_sem, ur_sem, rs_sem, rr_sem, lo_sem, gs_sem, gr_sem, ss_sem, sr_sem, wo_sem):
    problem, samp, feat = lax.axis_index("problem"), lax.axis_index("samp"), lax.axis_index("feat")
    partner = feat + 1 - 2 * lax.rem(feat, 2)
    mate = lax.rem(feat + 2, 4)
    cross = lax.rem(partner + 2, 4)
    to_partner, to_mate, to_cross = (problem, samp, partner), (problem, samp, mate), (problem, samp, cross)
    other = 1 - samp
    to_other = (problem, other, feat)

    owned = rb.shape[2]
    tile_rows = 4 * owned
    tiles = rb.shape[1]
    width = gb.shape[2]
    chunks = gr.shape[1]
    chunk = gb.shape[3]
    half_feats = chunks * chunk
    phases = GROUPS * (SWEEPS + 1)
    steps = tiles + EXTRA
    grad_end = tiles - 1 + LAG_GRAD
    total_rows = 2 * tiles * tile_rows

    def remote(src, dst, send, recv, device):
        return pltpu.make_async_remote_copy(src_ref=src, dst_ref=dst, send_sem=send, recv_sem=recv, device_id=device, device_id_type=MESH)

    barrier = pltpu.get_barrier_semaphore()
    for device in (to_partner, to_mate, to_cross, to_other):
        pl.semaphore_signal(barrier, inc=1, device_id=device, device_id_type=MESH)

    def load_tile(tile, slot):
        rows = pl.ds(pl.multiple_of(tile * tile_rows, tile_rows), tile_rows)
        return pltpu.make_async_copy(x_hbm.at[rows], xb.at[slot], x_sem.at[slot])

    own_feats = pl.ds(pl.multiple_of(samp * half_feats, half_feats), half_feats)
    first = [pltpu.make_async_copy(w0b_hbm.at[:, pl.ds(g * width, width)], sb.at[g], in_sem.at[g]) for g in range(GROUPS)]
    rest = [
        pltpu.make_async_copy(y_hbm.at[:, feat, :, pl.ds(g * width, width)], rb.at[g], in_sem.at[GROUPS + g])
        for g in range(GROUPS)
    ]
    rest += [
        pltpu.make_async_copy(w0_hbm.at[own_feats, pl.ds(g * width, width)], wb.at[g], in_sem.at[2 * GROUPS + g])
        for g in range(GROUPS)
    ]
    rest.append(pltpu.make_async_copy(eta_hbm.at[pl.ds(samp * chunks, chunks)], eb, in_sem.at[3 * GROUPS]))
    rest.append(pltpu.make_async_copy(lam_hbm, lb, in_sem.at[3 * GROUPS + 1]))
    first[0].start()
    load_tile(0, 0).start()
    for copy in first[1:] + rest:
        copy.start()
    for slot in range(1, RING):
        load_tile(slot, slot).start()
    for copy in first + rest:
        copy.wait()
    pl.semaphore_wait(barrier, 4)

    def product_copies(slot):
        return [
            remote(ub.at[slot, owner], ur.at[slot, rel], us_sem.at[slot, rel], ur_sem.at[slot, rel], device)
            for rel, (owner, device) in enumerate(((mate, to_mate), (cross, to_cross), (partner, to_partner)))
        ]

    def resid_rows(tile, owner, group):
        return r_out.at[
            pl.ds(pl.multiple_of(tile * tile_rows + owner * owned, owned), owned),
            pl.ds(pl.multiple_of(group * width, width), width),
        ]

    def resid_mate(slot):
        return remote(rt.at[slot, feat], rt.at[slot, feat], rs_sem.at[slot, 0], rr_sem.at[slot, 0], to_mate)

    def resid_partner(slot):
        return remote(rt.at[slot, feat], rt.at[slot, feat], rs_sem.at[slot, 1], rr_sem.at[slot, 1], to_partner)

    def resid_relay(slot):
        return remote(rt.at[slot, mate], rt.at[slot, mate], rs_sem.at[slot, 2], rr_sem.at[slot, 2], to_partner)

    def last_mate(slot, group, tile):
        return remote(rb.at[group, tile], fr.at[slot], rs_sem.at[slot, 0], rr_sem.at[slot, 0], to_mate)

    def last_partner(slot, group, tile):
        return remote(rb.at[group, tile], resid_rows(tile, feat, group), rs_sem.at[slot, 1], rr_sem.at[slot, 1], to_partner)

    def last_relay(slot, group, tile):
        return remote(fr.at[slot], resid_rows(tile, mate, group), rs_sem.at[slot, 2], rr_sem.at[slot, 2], to_partner)

    def last_own(slot, group, tile):
        return pltpu.make_async_copy(rb.at[group, tile], resid_rows(tile, feat, group), lo_sem.at[slot, 0])

    def last_mates(slot, group, tile):
        return pltpu.make_async_copy(fr.at[slot], resid_rows(tile, mate, group), lo_sem.at[slot, 1])

    def grad_copy(group, index):
        return remote(gb.at[group, other * chunks + index], gr.at[group, index], gs_sem.at[group, index], gr_sem.at[group, index], to_other)

    def delta_copy(group, index, count):
        rows = pl.ds(pl.multiple_of(samp * half_feats + index * chunk, chunk), count * chunk)
        return remote(sb.at[group, rows], sb.at[group, rows], ss_sem.at[group], sr_sem.at[group], to_other)

    def coef_rows(group):
        return w_out.at[own_feats, pl.ds(group * width, width)]

    def coef_remote(group):
        return remote(wb.at[group], coef_rows(group), wo_sem.at[group, 0], wo_sem.at[group, 1], to_other)

    def coef_local(group):
        return pltpu.make_async_copy(wb.at[group], coef_rows(group), wo_sem.at[group, 2])

    def step(g, carry):
        def at_lag(lag):
            moved = jnp.maximum(g - lag, 0)
            phase, tile = lax.div(moved, steps), lax.rem(moved, steps)
            active = (g >= lag) & (tile < tiles) & (phase < phases)
            slot = lax.rem(phase * tiles + tile, RING)
            return active, phase, lax.rem(phase, GROUPS), tile, slot

        moved = jnp.maximum(g - grad_end - FIRST_CHUNK, 0)
        chunk_phase, turn = lax.div(moved, steps), lax.rem(moved, steps)
        index = 3 * lax.div(turn, 4) + lax.rem(turn, 4)

        @pl.when((g >= grad_end + FIRST_CHUNK) & (chunk_phase < phases - GROUPS) & (lax.rem(turn, 4) < 3) & (index < chunks))
        def _():
            group = lax.rem(chunk_phase, GROUPS)
            grad_copy(group, index).wait()
            summed = gb[group, samp * chunks + index] + gr[group, index]
            gradient = summed.T * (1.0 / total_rows)
            rows = pl.ds(pl.multiple_of(index * chunk, chunk), chunk)
            coef = wb[group, rows]
            rate = jnp.broadcast_to(eb[index], (width, chunk)).T
            delta = rate * (gradient - lb[group] * coef)
            wb[group, rows] = coef + STEP_WEIGHT * delta
            sb[group, pl.ds(pl.multiple_of(samp * half_feats + index * chunk, chunk), chunk)] = delta.astype(jnp.bfloat16)
            delta_copy(group, index, 1).start()

            @pl.when((chunk_phase == phases - GROUPS - 1) & (index == chunks - 1))
            def _():
                for each in range(GROUPS):
                    coef_remote(each).start()
                    coef_local(each).start()

        active, phase, group, tile, slot = at_lag(LAG_RELAY)
        final = phase >= phases - GROUPS

        @pl.when(active & jnp.logical_not(final))
        def _():
            resid_mate(slot).wait_recv()
            resid_relay(slot).start()

        @pl.when(active & final)
        def _():
            last_mate(slot, group, tile).wait_recv()
            last_relay(slot, group, tile).start()
            last_mates(slot, group, tile).start()

        active_s, phase_s, group_s, tile_s, slot_s = at_lag(LAG_SUM)

        @pl.when(active_s)
        def _():
            for copy in product_copies(slot_s):
                copy.wait_recv()
            summed = ub[slot_s, feat].astype(jnp.float32) + ur[slot_s, 2].astype(jnp.float32)
            summed = summed + (ur[slot_s, 0].astype(jnp.float32) + ur[slot_s, 1].astype(jnp.float32))
            weight = jnp.where(phase_s < GROUPS, 1.0, STEP_WEIGHT)
            resid = rb[group_s, tile_s] - weight * summed
            rb[group_s, tile_s] = resid
            final_s = phase_s >= phases - GROUPS

            @pl.when(jnp.logical_not(final_s))
            def _():
                rt[slot_s, feat] = resid.astype(jnp.bfloat16).T
                resid_mate(slot_s).start()
                resid_partner(slot_s).start()

            @pl.when(final_s)
            def _():
                last_mate(slot_s, group_s, tile_s).start()
                last_partner(slot_s, group_s, tile_s).start()
                last_own(slot_s, group_s, tile_s).start()

        active_x, phase_x, group_x, tile_x, slot_x = at_lag(0)

        @pl.when(active_x & (tile_x == 0) & (phase_x >= GROUPS))
        def _():
            delta_copy(group_x, 0, chunks).wait()

        @pl.when(active_x)
        def _():
            load_tile(tile_x, slot_x).wait()
            product = jnp.dot(xb[slot_x], sb[group_x], preferred_element_type=jnp.float32)
            ub[slot_x] = product.astype(jnp.bfloat16).reshape(4, owned, width)
            for copy in product_copies(slot_x):
                copy.start()

        active_g, phase_g, group_g, tile_g, slot_g = at_lag(LAG_GRAD)
        final_g = phase_g >= phases - GROUPS

        @pl.when(active_g & jnp.logical_not(final_g))
        def _():
            resid_partner(slot_g).wait_recv()
            resid_relay(slot_g).wait_recv()
            left = jnp.concatenate([rt[slot_g, owner] for owner in range(4)], axis=1)
            for each in range(2 * chunks):
                part = jnp.dot(left, xb[slot_g, :, each * chunk:(each + 1) * chunk], preferred_element_type=jnp.float32)
                gb[group_g, each] = jnp.where(tile_g == 0, 0.0, gb[group_g, each]) + part

            @pl.when(tile_g == tiles - 1)
            def _():
                for each in range(chunks):
                    grad_copy(group_g, each).start()

            resid_mate(slot_g).wait_send()
            resid_partner(slot_g).wait_send()
            resid_relay(slot_g).wait_send()

        @pl.when(active_g & final_g)
        def _():
            last_partner(slot_g, group_g, tile_g).wait()
            last_relay(slot_g, group_g, tile_g).wait()
            last_mate(slot_g, group_g, tile_g).wait_send()
            last_own(slot_g, group_g, tile_g).wait()
            last_mates(slot_g, group_g, tile_g).wait()

        @pl.when(active_g)
        def _():
            for copy in product_copies(slot_g):
                copy.wait_send()
            ahead = phase_g * tiles + tile_g + RING

            @pl.when(ahead < phases * tiles)
            def _():
                load_tile(lax.rem(ahead, tiles), slot_g).start()

        return carry

    lax.fori_loop(0, (phases - 1) * steps + tiles + LAG_GRAD, step, 0)
    for group in range(GROUPS):
        coef_remote(group).wait()
        coef_local(group).wait()


def sweeps(design, targets, coef_init, step_sizes, ridge_weights):
    rows, feats = design.shape
    width = targets.shape[1] // GROUPS
    owned = 128
    tiles = rows // (4 * owned)
    chunks = 8
    chunk = feats // (2 * chunks)
    dma = pltpu.SemaphoreType.DMA
    f32, bf16 = jnp.float32, jnp.bfloat16
    scratch = [
        pltpu.VMEM((RING, 4 * owned, feats), bf16),
        pltpu.VMEM((GROUPS, feats, width), bf16),
        pltpu.VMEM((GROUPS, 2 * chunks, width, chunk), f32),
        pltpu.VMEM((GROUPS, chunks, width, chunk), f32),
        pltpu.VMEM((GROUPS, feats // 2, width), f32),
        pltpu.VMEM((chunks, 1, chunk), f32),
        pltpu.VMEM((GROUPS, 1, width), f32),
        pltpu.VMEM((GROUPS, tiles, owned, width), f32),
        pltpu.VMEM((RING, 4, width, owned), bf16),
        pltpu.VMEM((RING, 4, owned, width), bf16),
        pltpu.VMEM((RING, 3, owned, width), bf16),
        pltpu.VMEM((RING, owned, width), f32),
        dma((RING,)),
        dma((3 * GROUPS + 2,)),
        dma((RING, 3)),
        dma((RING, 3)),
        dma((RING, 3)),
        dma((RING, 3)),
        dma((RING, 2)),
        dma((GROUPS, chunks)),
        dma((GROUPS, chunks)),
        dma((GROUPS,)),
        dma((GROUPS,)),
        dma((GROUPS, 3)),
    ]
    return pl.pallas_call(
        kernel,
        out_shape=(jax.ShapeDtypeStruct(coef_init.shape, f32), jax.ShapeDtypeStruct(targets.shape, f32)),
        in_specs=[pl.BlockSpec(memory_space=pl.ANY)] * 6,
        out_specs=[pl.BlockSpec(memory_space=pl.ANY)] * 2,
        scratch_shapes=scratch,
        compiler_params=pltpu.CompilerParams(collective_id=0, has_side_effects=True, vmem_limit_bytes=60 * 2**20),
    )(
        design,
        targets.reshape(tiles, 4, owned, targets.shape[1]),
        coef_init,
        coef_init.astype(bf16),
        step_sizes.reshape(2 * chunks, 1, chunk),
        ridge_weights.reshape(GROUPS, 1, width),
    )


def solution(mesh):
    design_spec = P(("problem", "samp"), "feat")
    rows_spec = P(("problem", "samp"), None)
    coef_spec = P(("problem", "feat"), None)
    step_spec = P(("problem", "feat"))
    ridge_spec = P("problem")
    return jax.shard_map(sweeps, mesh=mesh, in_specs=(design_spec, rows_spec, coef_spec, step_spec, ridge_spec), out_specs=(coef_spec, rows_spec), check_vma=False)
```

```python
import functools

import jax
import jax.numpy as jnp
from jax import lax
from jax.experimental import pallas as pl
from jax.experimental.pallas import tpu as pltpu
from jax.sharding import PartitionSpec as P

SWEEPS = 4
STEP_WEIGHT = 0.5
MESH = pl.DeviceIdType.MESH

RING = 10
LAG_SUM = 3
LAG_RELAY = 7
LAG_GRAD = 8
EXTRA = 6
FIRST_CHUNK = 5
CHUNK_TURNS = (2, 3)
GROUPS = 2


def kernel(x_hbm, y_hbm, w0_hbm, eta_hbm, lam_hbm, w_out, r_out,
           xb, sb, st, gb, gr, wb, eb, lb, rb, rt, ub, ur, fr,
           x_sem, in_sem, us_sem, ur_sem, rs_sem, rr_sem, lo_sem, gs_sem, gr_sem, ss_sem, sr_sem, wo_sem):
    problem, samp, feat = lax.axis_index("problem"), lax.axis_index("samp"), lax.axis_index("feat")
    partner = feat + 1 - 2 * lax.rem(feat, 2)
    mate = lax.rem(feat + 2, 4)
    cross = lax.rem(partner + 2, 4)
    to_partner, to_mate, to_cross = (problem, samp, partner), (problem, samp, mate), (problem, samp, cross)
    other = 1 - samp
    to_other = (problem, other, feat)

    owned = rb.shape[2]
    tile_rows = 4 * owned
    tiles = rb.shape[1]
    width = gb.shape[2]
    chunks = gr.shape[1]
    chunk = gb.shape[3]
    half_feats = chunks * chunk
    phases = GROUPS * (SWEEPS + 1)
    steps = tiles + EXTRA
    grad_end = tiles - 1 + LAG_GRAD
    total_rows = 2 * tiles * tile_rows

    def remote(src, dst, send, recv, device):
        return pltpu.make_async_remote_copy(src_ref=src, dst_ref=dst, send_sem=send, recv_sem=recv, device_id=device, device_id_type=MESH)

    barrier = pltpu.get_barrier_semaphore()
    for device in (to_partner, to_mate, to_cross, to_other):
        pl.semaphore_signal(barrier, inc=1, device_id=device, device_id_type=MESH)

    def load_tile(tile, slot):
        rows = pl.ds(pl.multiple_of(tile * tile_rows, tile_rows), tile_rows)
        return pltpu.make_async_copy(x_hbm.at[rows], xb.at[slot], x_sem.at[slot])

    own_feats = pl.ds(pl.multiple_of(samp * half_feats, half_feats), half_feats)
    other_feats = pl.ds(pl.multiple_of(other * half_feats, half_feats), half_feats)

    def own_coef(group):
        return pltpu.make_async_copy(w0_hbm.at[own_feats, pl.ds(group * width, width)], wb.at[group], in_sem.at[group])

    def other_coef(group):
        return pltpu.make_async_copy(w0_hbm.at[other_feats, pl.ds(group * width, width)], st, in_sem.at[GROUPS + group])

    def round_coef(group):
        own_coef(group).wait()
        other_coef(group).wait()
        for each in range(chunks):
            rows = pl.ds(each * chunk, chunk)
            for start, source in ((samp, wb.at[group]), (other, st)):
                target = pl.ds(pl.multiple_of(start * half_feats + each * chunk, chunk), chunk)
                sb[group, target] = source[rows].astype(jnp.bfloat16)

    rest = [
        pltpu.make_async_copy(y_hbm.at[:, feat, :, pl.ds(g * width, width)], rb.at[g], in_sem.at[2 * GROUPS + g])
        for g in range(GROUPS)
    ]
    rest.append(pltpu.make_async_copy(eta_hbm.at[pl.ds(samp * chunks, chunks)], eb, in_sem.at[3 * GROUPS]))
    rest.append(pltpu.make_async_copy(lam_hbm, lb, in_sem.at[3 * GROUPS + 1]))
    own_coef(0).start()
    other_coef(0).start()
    load_tile(0, 0).start()
    load_tile(1, 1).start()
    for copy in rest:
        copy.start()
    own_coef(1).start()
    for slot in range(2, RING):
        load_tile(slot, slot).start()
    round_coef(0)
    other_coef(1).start()
    for copy in rest:
        copy.wait()
    pl.semaphore_wait(barrier, 4)

    def product_copies(slot):
        return [
            remote(ub.at[slot, owner], ur.at[slot, rel], us_sem.at[slot, rel], ur_sem.at[slot, rel], device)
            for rel, (owner, device) in enumerate(((mate, to_mate), (cross, to_cross), (partner, to_partner)))
        ]

    def resid_rows(tile, owner, group):
        return r_out.at[
            pl.ds(pl.multiple_of(tile * tile_rows + owner * owned, owned), owned),
            pl.ds(pl.multiple_of(group * width, width), width),
        ]

    def resid_mate(slot):
        return remote(rt.at[slot, feat], rt.at[slot, feat], rs_sem.at[slot, 0], rr_sem.at[slot, 0], to_mate)

    def resid_partner(slot):
        return remote(rt.at[slot, feat], rt.at[slot, feat], rs_sem.at[slot, 1], rr_sem.at[slot, 1], to_partner)

    def resid_relay(slot):
        return remote(rt.at[slot, mate], rt.at[slot, mate], rs_sem.at[slot, 2], rr_sem.at[slot, 2], to_partner)

    def last_mate(slot, group, tile):
        return remote(rb.at[group, tile], fr.at[slot], rs_sem.at[slot, 0], rr_sem.at[slot, 0], to_mate)

    def last_partner(slot, group, tile):
        return remote(rb.at[group, tile], resid_rows(tile, feat, group), rs_sem.at[slot, 1], rr_sem.at[slot, 1], to_partner)

    def last_relay(slot, group, tile):
        return remote(fr.at[slot], resid_rows(tile, mate, group), rs_sem.at[slot, 2], rr_sem.at[slot, 2], to_partner)

    def last_own(slot, group, tile):
        return pltpu.make_async_copy(rb.at[group, tile], resid_rows(tile, feat, group), lo_sem.at[slot, 0])

    def last_mates(slot, group, tile):
        return pltpu.make_async_copy(fr.at[slot], resid_rows(tile, mate, group), lo_sem.at[slot, 1])

    def grad_copy(group, index):
        return remote(gb.at[group, other * chunks + index], gr.at[group, index], gs_sem.at[group, index], gr_sem.at[group, index], to_other)

    def delta_copy(group, index, count):
        rows = pl.ds(pl.multiple_of(samp * half_feats + index * chunk, chunk), count * chunk)
        return remote(sb.at[group, rows], sb.at[group, rows], ss_sem.at[group], sr_sem.at[group], to_other)

    def coef_rows(group):
        return w_out.at[own_feats, pl.ds(group * width, width)]

    def coef_remote(group):
        return remote(wb.at[group], coef_rows(group), wo_sem.at[group, 0], wo_sem.at[group, 1], to_other)

    def coef_local(group):
        return pltpu.make_async_copy(wb.at[group], coef_rows(group), wo_sem.at[group, 2])

    def step(g, carry):
        def at_lag(lag):
            moved = jnp.maximum(g - lag, 0)
            phase, tile = lax.div(moved, steps), lax.rem(moved, steps)
            active = (g >= lag) & (tile < tiles) & (phase < phases)
            slot = lax.rem(phase * tiles + tile, RING)
            return active, phase, lax.rem(phase, GROUPS), tile, slot

        active_x, phase_x, group_x, tile_x, slot_x = at_lag(0)

        @pl.when(active_x & (tile_x == 0) & (phase_x >= GROUPS))
        def _():
            delta_copy(group_x, 0, chunks).wait()

        @pl.when(active_x & (tile_x == 0) & (phase_x == 1))
        def _():
            round_coef(1)

        @pl.when(active_x)
        def _():
            load_tile(tile_x, slot_x).wait()
            product = jnp.dot(xb[slot_x], sb[group_x], preferred_element_type=jnp.float32)
            ub[slot_x] = product.astype(jnp.bfloat16).reshape(4, owned, width)
            for copy in product_copies(slot_x):
                copy.start()

        active, phase, group, tile, slot = at_lag(LAG_RELAY)
        final = phase >= phases - GROUPS

        @pl.when(active & jnp.logical_not(final))
        def _():
            resid_mate(slot).wait_recv()
            resid_relay(slot).start()

        @pl.when(active & final)
        def _():
            last_mate(slot, group, tile).wait_recv()
            last_relay(slot, group, tile).start()
            last_mates(slot, group, tile).start()

        active_s, phase_s, group_s, tile_s, slot_s = at_lag(LAG_SUM)

        @pl.when(active_s)
        def _():
            for copy in product_copies(slot_s):
                copy.wait_recv()
            summed = ub[slot_s, feat].astype(jnp.float32) + ur[slot_s, 2].astype(jnp.float32)
            summed = summed + (ur[slot_s, 0].astype(jnp.float32) + ur[slot_s, 1].astype(jnp.float32))
            weight = jnp.where(phase_s < GROUPS, 1.0, STEP_WEIGHT)
            resid = rb[group_s, tile_s] - weight * summed
            rb[group_s, tile_s] = resid
            final_s = phase_s >= phases - GROUPS

            @pl.when(jnp.logical_not(final_s))
            def _():
                rt[slot_s, feat] = resid.astype(jnp.bfloat16).T
                resid_mate(slot_s).start()
                resid_partner(slot_s).start()

            @pl.when(final_s)
            def _():
                last_mate(slot_s, group_s, tile_s).start()
                last_partner(slot_s, group_s, tile_s).start()
                last_own(slot_s, group_s, tile_s).start()

        moved = jnp.maximum(g - grad_end - FIRST_CHUNK, 0)
        chunk_phase, turn = lax.div(moved, steps), lax.rem(moved, steps)
        index = CHUNK_TURNS[0] * lax.div(turn, CHUNK_TURNS[1]) + lax.rem(turn, CHUNK_TURNS[1])

        @pl.when((g >= grad_end + FIRST_CHUNK) & (chunk_phase < phases - GROUPS) & (lax.rem(turn, CHUNK_TURNS[1]) < CHUNK_TURNS[0]) & (index < chunks))
        def _():
            group = lax.rem(chunk_phase, GROUPS)
            grad_copy(group, index).wait()
            summed = gb[group, samp * chunks + index] + gr[group, index]
            gradient = summed.T * (1.0 / total_rows)
            rows = pl.ds(pl.multiple_of(index * chunk, chunk), chunk)
            coef = wb[group, rows]
            rate = jnp.broadcast_to(eb[index], (width, chunk)).T
            delta = rate * (gradient - lb[group] * coef)
            wb[group, rows] = coef + STEP_WEIGHT * delta
            sb[group, pl.ds(pl.multiple_of(samp * half_feats + index * chunk, chunk), chunk)] = delta.astype(jnp.bfloat16)
            delta_copy(group, index, 1).start()

            @pl.when((chunk_phase == phases - GROUPS - 1) & (index == chunks - 1))
            def _():
                for each in range(GROUPS):
                    coef_remote(each).start()
                    coef_local(each).start()

        active_g, phase_g, group_g, tile_g, slot_g = at_lag(LAG_GRAD)
        final_g = phase_g >= phases - GROUPS

        @pl.when(active_g & jnp.logical_not(final_g))
        def _():
            resid_partner(slot_g).wait_recv()
            resid_relay(slot_g).wait_recv()
            left = jnp.concatenate([rt[slot_g, owner] for owner in range(4)], axis=1)
            for each in range(2 * chunks):
                part = jnp.dot(left, xb[slot_g, :, each * chunk:(each + 1) * chunk], preferred_element_type=jnp.float32)
                gb[group_g, each] = jnp.where(tile_g == 0, 0.0, gb[group_g, each]) + part

            @pl.when(tile_g == tiles - 1)
            def _():
                for each in range(chunks):
                    grad_copy(group_g, each).start()

            resid_mate(slot_g).wait_send()
            resid_partner(slot_g).wait_send()
            resid_relay(slot_g).wait_send()

        @pl.when(active_g & final_g)
        def _():
            last_partner(slot_g, group_g, tile_g).wait()
            last_relay(slot_g, group_g, tile_g).wait()
            last_mate(slot_g, group_g, tile_g).wait_send()
            last_own(slot_g, group_g, tile_g).wait()
            last_mates(slot_g, group_g, tile_g).wait()

        @pl.when(active_g)
        def _():
            for copy in product_copies(slot_g):
                copy.wait_send()
            ahead = phase_g * tiles + tile_g + RING

            @pl.when(ahead < phases * tiles)
            def _():
                load_tile(lax.rem(ahead, tiles), slot_g).start()

        return carry

    lax.fori_loop(0, (phases - 1) * steps + tiles + LAG_GRAD, step, 0)
    for group in range(GROUPS):
        coef_remote(group).wait()
        coef_local(group).wait()


def sweeps(design, targets, coef_init, step_sizes, ridge_weights):
    rows, feats = design.shape
    width = targets.shape[1] // GROUPS
    owned = 128
    tiles = rows // (4 * owned)
    chunks = 8
    chunk = feats // (2 * chunks)
    dma = pltpu.SemaphoreType.DMA
    f32, bf16 = jnp.float32, jnp.bfloat16
    scratch = [
        pltpu.VMEM((RING, 4 * owned, feats), bf16),
        pltpu.VMEM((GROUPS, feats, width), bf16),
        pltpu.VMEM((feats // 2, width), f32),
        pltpu.VMEM((GROUPS, 2 * chunks, width, chunk), f32),
        pltpu.VMEM((GROUPS, chunks, width, chunk), f32),
        pltpu.VMEM((GROUPS, feats // 2, width), f32),
        pltpu.VMEM((chunks, 1, chunk), f32),
        pltpu.VMEM((GROUPS, 1, width), f32),
        pltpu.VMEM((GROUPS, tiles, owned, width), f32),
        pltpu.VMEM((RING, 4, width, owned), bf16),
        pltpu.VMEM((RING, 4, owned, width), bf16),
        pltpu.VMEM((RING, 3, owned, width), bf16),
        pltpu.VMEM((RING, owned, width), f32),
        dma((RING,)),
        dma((3 * GROUPS + 2,)),
        dma((RING, 3)),
        dma((RING, 3)),
        dma((RING, 3)),
        dma((RING, 3)),
        dma((RING, 2)),
        dma((GROUPS, chunks)),
        dma((GROUPS, chunks)),
        dma((GROUPS,)),
        dma((GROUPS,)),
        dma((GROUPS, 3)),
    ]
    return pl.pallas_call(
        kernel,
        out_shape=(jax.ShapeDtypeStruct(coef_init.shape, f32), jax.ShapeDtypeStruct(targets.shape, f32)),
        in_specs=[pl.BlockSpec(memory_space=pl.ANY)] * 5,
        out_specs=[pl.BlockSpec(memory_space=pl.ANY)] * 2,
        scratch_shapes=scratch,
        compiler_params=pltpu.CompilerParams(collective_id=0, has_side_effects=True, vmem_limit_bytes=63 * 2**20),
    )(
        design,
        targets.reshape(tiles, 4, owned, targets.shape[1]),
        coef_init,
        step_sizes.reshape(2 * chunks, 1, chunk),
        ridge_weights.reshape(GROUPS, 1, width),
    )


def solution(mesh):
    design_spec = P(("problem", "samp"), "feat")
    rows_spec = P(("problem", "samp"), None)
    coef_spec = P(("problem", "feat"), None)
    step_spec = P(("problem", "feat"))
    ridge_spec = P("problem")
    return jax.shard_map(sweeps, mesh=mesh, in_specs=(design_spec, rows_spec, coef_spec, step_spec, ridge_spec), out_specs=(coef_spec, rows_spec), check_vma=False)
```

```python
import functools

import jax
import jax.numpy as jnp
from jax import lax
from jax.experimental import pallas as pl
from jax.experimental.pallas import tpu as pltpu
from jax.sharding import PartitionSpec as P

SWEEPS = 4
STEP_WEIGHT = 0.5
MESH = pl.DeviceIdType.MESH

RING = 10
ORDER = "yroxg"
SWEEP_WORK = "yrgryrgrogrgyorggorgrggrxgxxxoxooxyxroxyrxroggyogoxxrxrgrxogyrgoyoooxxox"
LAST_WORK = "yrgrygryrgroggrogogxxxxrrxgooorgogxyrrroxroxrxgxoyyxoyoggxgorxgxrygxooox"
BEHIND = {"r": 9, "o": 3, "g": 10, "y": 11, "x": 0}
GROUPS = 2


def pack(work):
    ranks = [ORDER.index(letter) for letter in work]
    step, words, last = 0, {letter: [0, 0] for letter in ORDER}, -1
    for rank, letter in zip(ranks, work):
        if rank <= last:
            step += 1
        last = rank
        words[letter][step // 31] |= 1 << (step % 31)
    return step + 1, words


def count_steps(tiles, chunks, phases, lengths):
    total = 0
    for phase in range(phases + 2):
        work = SWEEP_WORK if phase < phases - GROUPS else LAST_WORK
        need = {letter: phases * tiles + BEHIND[letter] for letter in "xorg"}
        need["y"] = (phases - GROUPS) * chunks + BEHIND["y"]
        done = {letter: min(phase, phases - GROUPS) * SWEEP_WORK.count(letter) + max(phase - phases + GROUPS, 0) * LAST_WORK.count(letter) for letter in need}
        if all(done[letter] >= need[letter] for letter in need):
            break
        total += lengths[phase >= phases - GROUPS]
    return total


def kernel(x_hbm, y_hbm, w0_hbm, eta_hbm, lam_hbm, w_out, r_out,
           xb, sb, st, gb, gr, wb, eb, lb, rb, rt, ub, ur, fr,
           x_sem, in_sem, us_sem, ur_sem, rs_sem, rr_sem, lo_sem, gs_sem, gr_sem, ss_sem, sr_sem, wo_sem):
    problem, samp, feat = lax.axis_index("problem"), lax.axis_index("samp"), lax.axis_index("feat")
    partner = feat + 1 - 2 * lax.rem(feat, 2)
    mate = lax.rem(feat + 2, 4)
    cross = lax.rem(partner + 2, 4)
    to_partner, to_mate, to_cross = (problem, samp, partner), (problem, samp, mate), (problem, samp, cross)
    other = 1 - samp
    to_other = (problem, other, feat)

    owned = rb.shape[2]
    tile_rows = 4 * owned
    tiles = rb.shape[1]
    width = gb.shape[2]
    chunks = gr.shape[1]
    chunk = gb.shape[3]
    half_feats = chunks * chunk
    phases = GROUPS * (SWEEPS + 1)
    (sweep_steps, sweep_words), (last_steps, last_words) = pack(SWEEP_WORK), pack(LAST_WORK)
    total_rows = 2 * tiles * tile_rows

    def remote(src, dst, send, recv, device):
        return pltpu.make_async_remote_copy(src_ref=src, dst_ref=dst, send_sem=send, recv_sem=recv, device_id=device, device_id_type=MESH)

    barrier = pltpu.get_barrier_semaphore()
    for device in (to_partner, to_mate, to_cross, to_other):
        pl.semaphore_signal(barrier, inc=1, device_id=device, device_id_type=MESH)

    def load_tile(tile, slot):
        rows = pl.ds(pl.multiple_of(tile * tile_rows, tile_rows), tile_rows)
        return pltpu.make_async_copy(x_hbm.at[rows], xb.at[slot], x_sem.at[slot])

    own_feats = pl.ds(pl.multiple_of(samp * half_feats, half_feats), half_feats)
    other_feats = pl.ds(pl.multiple_of(other * half_feats, half_feats), half_feats)

    def own_coef(group):
        return pltpu.make_async_copy(w0_hbm.at[own_feats, pl.ds(group * width, width)], wb.at[group], in_sem.at[group])

    def other_coef(group):
        return pltpu.make_async_copy(w0_hbm.at[other_feats, pl.ds(group * width, width)], st, in_sem.at[GROUPS + group])

    def round_coef(group):
        own_coef(group).wait()
        other_coef(group).wait()
        for each in range(chunks):
            rows = pl.ds(each * chunk, chunk)
            for start, source in ((samp, wb.at[group]), (other, st)):
                target = pl.ds(pl.multiple_of(start * half_feats + each * chunk, chunk), chunk)
                sb[group, target] = source[rows].astype(jnp.bfloat16)

    rest = [
        pltpu.make_async_copy(y_hbm.at[:, feat, :, pl.ds(g * width, width)], rb.at[g], in_sem.at[2 * GROUPS + g])
        for g in range(GROUPS)
    ]
    rest.append(pltpu.make_async_copy(eta_hbm.at[pl.ds(samp * chunks, chunks)], eb, in_sem.at[3 * GROUPS]))
    rest.append(pltpu.make_async_copy(lam_hbm, lb, in_sem.at[3 * GROUPS + 1]))
    own_coef(0).start()
    other_coef(0).start()
    load_tile(0, 0).start()
    load_tile(1, 1).start()
    for copy in rest:
        copy.start()
    own_coef(1).start()
    for slot in range(2, RING):
        load_tile(slot, slot).start()
    round_coef(0)
    other_coef(1).start()
    for copy in rest:
        copy.wait()
    pl.semaphore_wait(barrier, 4)

    def product_copies(slot):
        return [
            remote(ub.at[slot, owner], ur.at[slot, rel], us_sem.at[slot, rel], ur_sem.at[slot, rel], device)
            for rel, (owner, device) in enumerate(((mate, to_mate), (cross, to_cross), (partner, to_partner)))
        ]

    def resid_rows(tile, owner, group):
        return r_out.at[
            pl.ds(pl.multiple_of(tile * tile_rows + owner * owned, owned), owned),
            pl.ds(pl.multiple_of(group * width, width), width),
        ]

    def resid_mate(slot):
        return remote(rt.at[slot, feat], rt.at[slot, feat], rs_sem.at[slot, 0], rr_sem.at[slot, 0], to_mate)

    def resid_partner(slot):
        return remote(rt.at[slot, feat], rt.at[slot, feat], rs_sem.at[slot, 1], rr_sem.at[slot, 1], to_partner)

    def resid_relay(slot):
        return remote(rt.at[slot, mate], rt.at[slot, mate], rs_sem.at[slot, 2], rr_sem.at[slot, 2], to_partner)

    def last_mate(slot, group, tile):
        return remote(rb.at[group, tile], fr.at[slot], rs_sem.at[slot, 0], rr_sem.at[slot, 0], to_mate)

    def last_partner(slot, group, tile):
        return remote(rb.at[group, tile], resid_rows(tile, feat, group), rs_sem.at[slot, 1], rr_sem.at[slot, 1], to_partner)

    def last_relay(slot, group, tile):
        return remote(fr.at[slot], resid_rows(tile, mate, group), rs_sem.at[slot, 2], rr_sem.at[slot, 2], to_partner)

    def last_own(slot, group, tile):
        return pltpu.make_async_copy(rb.at[group, tile], resid_rows(tile, feat, group), lo_sem.at[slot, 0])

    def last_mates(slot, group, tile):
        return pltpu.make_async_copy(fr.at[slot], resid_rows(tile, mate, group), lo_sem.at[slot, 1])

    def grad_copy(group, index):
        return remote(gb.at[group, other * chunks + index], gr.at[group, index], gs_sem.at[group, index], gr_sem.at[group, index], to_other)

    def delta_copy(group, index, count):
        rows = pl.ds(pl.multiple_of(samp * half_feats + index * chunk, chunk), count * chunk)
        return remote(sb.at[group, rows], sb.at[group, rows], ss_sem.at[group], sr_sem.at[group], to_other)

    def coef_rows(group):
        return w_out.at[own_feats, pl.ds(group * width, width)]

    def coef_remote(group):
        return remote(wb.at[group], coef_rows(group), wo_sem.at[group, 0], wo_sem.at[group, 1], to_other)

    def coef_local(group):
        return pltpu.make_async_copy(wb.at[group], coef_rows(group), wo_sem.at[group, 2])

    def step(_, carry):
        turn, period, states = carry
        ending = period >= phases - GROUPS
        bits = {}
        for letter in ORDER:
            early = jnp.where(ending, jnp.int32(last_words[letter][0]), jnp.int32(sweep_words[letter][0]))
            late = jnp.where(ending, jnp.int32(last_words[letter][1]), jnp.int32(sweep_words[letter][1]))
            word = jnp.where(turn < 31, early, late)
            bits[letter] = lax.shift_right_logical(word, jnp.where(turn < 31, turn, turn - 31)) & 1

        def turn_of(letter):
            tile, phase, slot = states[letter]
            active = (bits[letter] == 1) & (tile >= 0) & (phase < phases)
            return active, phase >= phases - GROUPS, phase, phase & 1, tile, slot

        active_x, _, phase_x, group_x, tile_x, slot_x = turn_of("x")
        active, final, phase, group, tile, slot = turn_of("r")
        active_s, final_s, phase_s, group_s, tile_s, slot_s = turn_of("o")
        active_g, final_g, phase_g, group_g, tile_g, slot_g = turn_of("g")
        index, chunk_phase, _ = states["y"]

        @pl.when((bits["y"] == 1) & (index >= 0) & (chunk_phase < phases - GROUPS))
        def _():
            group = chunk_phase & 1
            grad_copy(group, index).wait()
            summed = gb[group, samp * chunks + index] + gr[group, index]
            gradient = summed.T * (1.0 / total_rows)
            rows = pl.ds(pl.multiple_of(index * chunk, chunk), chunk)
            coef = wb[group, rows]
            rate = jnp.broadcast_to(eb[index], (width, chunk)).T
            delta = rate * (gradient - lb[group] * coef)
            wb[group, rows] = coef + STEP_WEIGHT * delta
            sb[group, pl.ds(pl.multiple_of(samp * half_feats + index * chunk, chunk), chunk)] = delta.astype(jnp.bfloat16)
            delta_copy(group, index, 1).start()

            @pl.when((chunk_phase == phases - GROUPS - 1) & (index == chunks - 1))
            def _():
                for each in range(GROUPS):
                    coef_remote(each).start()
                    coef_local(each).start()

        @pl.when(active & jnp.logical_not(final))
        def _():
            resid_mate(slot).wait_recv()
            resid_relay(slot).start()

        @pl.when(active & final)
        def _():
            last_mate(slot, group, tile).wait_recv()
            last_relay(slot, group, tile).start()
            last_mates(slot, group, tile).start()

        @pl.when(active_s)
        def _():
            for copy in product_copies(slot_s):
                copy.wait_recv()
            summed = ub[slot_s, feat].astype(jnp.float32) + ur[slot_s, 2].astype(jnp.float32)
            summed = summed + (ur[slot_s, 0].astype(jnp.float32) + ur[slot_s, 1].astype(jnp.float32))
            weight = jnp.where(phase_s < GROUPS, 1.0, STEP_WEIGHT)
            resid = rb[group_s, tile_s] - weight * summed
            rb[group_s, tile_s] = resid

            @pl.when(jnp.logical_not(final_s))
            def _():
                rt[slot_s, feat] = resid.astype(jnp.bfloat16).T
                resid_mate(slot_s).start()
                resid_partner(slot_s).start()

            @pl.when(final_s)
            def _():
                last_mate(slot_s, group_s, tile_s).start()
                last_partner(slot_s, group_s, tile_s).start()
                last_own(slot_s, group_s, tile_s).start()

        @pl.when(active_x & (tile_x == 0) & (phase_x >= GROUPS))
        def _():
            delta_copy(group_x, 0, chunks).wait()

        @pl.when(active_x & (tile_x == 0) & (phase_x == 1))
        def _():
            round_coef(1)

        @pl.when(active_x)
        def _():
            load_tile(tile_x, slot_x).wait()
            product = jnp.dot(xb[slot_x], sb[group_x], preferred_element_type=jnp.float32)
            ub[slot_x] = product.astype(jnp.bfloat16).reshape(4, owned, width)
            for copy in product_copies(slot_x):
                copy.start()

        @pl.when(active_g & jnp.logical_not(final_g))
        def _():
            resid_partner(slot_g).wait_recv()
            resid_relay(slot_g).wait_recv()

            @pl.when(tile_g < tiles - 1)
            def _():
                left = jnp.concatenate([rt[slot_g, owner] for owner in range(4)], axis=1)
                for each in range(2 * chunks):
                    share = jnp.dot(left, xb[slot_g, :, each * chunk:(each + 1) * chunk], preferred_element_type=jnp.float32)
                    gb[group_g, each] = jnp.where(tile_g == 0, 0.0, gb[group_g, each]) + share

            @pl.when(tile_g == tiles - 1)
            def _():
                left = jnp.concatenate([rt[slot_g, owner] for owner in range(4)], axis=1)
                for side in (other, samp):
                    for each in range(chunks):
                        feats = pl.ds(pl.multiple_of((side * chunks + each) * chunk, chunk), chunk)
                        share = jnp.dot(left, xb[slot_g, :, feats], preferred_element_type=jnp.float32)
                        gb[group_g, side * chunks + each] += share
                    if side is other:
                        for each in range(chunks):
                            grad_copy(group_g, each).start()

            resid_mate(slot_g).wait_send()
            resid_partner(slot_g).wait_send()
            resid_relay(slot_g).wait_send()

        @pl.when(active_g & final_g)
        def _():
            last_partner(slot_g, group_g, tile_g).wait()
            last_relay(slot_g, group_g, tile_g).wait()
            last_mate(slot_g, group_g, tile_g).wait_send()
            last_own(slot_g, group_g, tile_g).wait()
            last_mates(slot_g, group_g, tile_g).wait()

        @pl.when(active_g)
        def _():
            for copy in product_copies(slot_g):
                copy.wait_send()

            @pl.when(phase_g * tiles + tile_g + RING < phases * tiles)
            def _():
                ahead = jnp.where(tile_g + RING >= tiles, tile_g + RING - tiles, tile_g + RING)
                load_tile(ahead, slot_g).start()

        following = {}
        for letter in ORDER:
            tile, phase, slot = states[letter]
            slot = jnp.where((bits[letter] == 1) & (tile >= 0), slot + 1, slot)
            tile = tile + bits[letter]
            wrap = tile == (chunks if letter == "y" else tiles)
            following[letter] = (
                jnp.where(wrap, 0, tile),
                jnp.where(wrap, phase + 1, phase),
                jnp.where(slot == RING, 0, slot),
            )
        wrap = turn == jnp.where(ending, last_steps - 1, sweep_steps - 1)
        return jnp.where(wrap, 0, turn + 1), jnp.where(wrap, period + 1, period), following

    zero = jnp.int32(0)
    start = {letter: (jnp.int32(-BEHIND[letter]), zero, zero) for letter in ORDER}
    lax.fori_loop(0, count_steps(tiles, chunks, phases, (sweep_steps, last_steps)), step, (zero, zero, start))
    for group in range(GROUPS):
        coef_remote(group).wait()
        coef_local(group).wait()


def sweeps(design, targets, coef_init, step_sizes, ridge_weights):
    rows, feats = design.shape
    width = targets.shape[1] // GROUPS
    owned = 128
    tiles = rows // (4 * owned)
    chunks = 8
    chunk = feats // (2 * chunks)
    dma = pltpu.SemaphoreType.DMA
    f32, bf16 = jnp.float32, jnp.bfloat16
    scratch = [
        pltpu.VMEM((RING, 4 * owned, feats), bf16),
        pltpu.VMEM((GROUPS, feats, width), bf16),
        pltpu.VMEM((feats // 2, width), f32),
        pltpu.VMEM((GROUPS, 2 * chunks, width, chunk), f32),
        pltpu.VMEM((GROUPS, chunks, width, chunk), f32),
        pltpu.VMEM((GROUPS, feats // 2, width), f32),
        pltpu.VMEM((chunks, 1, chunk), f32),
        pltpu.VMEM((GROUPS, 1, width), f32),
        pltpu.VMEM((GROUPS, tiles, owned, width), f32),
        pltpu.VMEM((RING, 4, width, owned), bf16),
        pltpu.VMEM((RING, 4, owned, width), bf16),
        pltpu.VMEM((RING, 3, owned, width), bf16),
        pltpu.VMEM((RING, owned, width), f32),
        dma((RING,)),
        dma((3 * GROUPS + 2,)),
        dma((RING, 3)),
        dma((RING, 3)),
        dma((RING, 3)),
        dma((RING, 3)),
        dma((RING, 2)),
        dma((GROUPS, chunks)),
        dma((GROUPS, chunks)),
        dma((GROUPS,)),
        dma((GROUPS,)),
        dma((GROUPS, 3)),
    ]
    return pl.pallas_call(
        kernel,
        out_shape=(jax.ShapeDtypeStruct(coef_init.shape, f32), jax.ShapeDtypeStruct(targets.shape, f32)),
        in_specs=[pl.BlockSpec(memory_space=pl.ANY)] * 5,
        out_specs=[pl.BlockSpec(memory_space=pl.ANY)] * 2,
        scratch_shapes=scratch,
        compiler_params=pltpu.CompilerParams(collective_id=0, has_side_effects=True, vmem_limit_bytes=63 * 2**20),
    )(
        design,
        targets.reshape(tiles, 4, owned, targets.shape[1]),
        coef_init,
        step_sizes.reshape(2 * chunks, 1, chunk),
        ridge_weights.reshape(GROUPS, 1, width),
    )


def solution(mesh):
    design_spec = P(("problem", "samp"), "feat")
    rows_spec = P(("problem", "samp"), None)
    coef_spec = P(("problem", "feat"), None)
    step_spec = P(("problem", "feat"))
    ridge_spec = P("problem")
    return jax.shard_map(sweeps, mesh=mesh, in_specs=(design_spec, rows_spec, coef_spec, step_spec, ridge_spec), out_specs=(coef_spec, rows_spec), check_vma=False)
```

```python
import functools

import jax
import jax.numpy as jnp
from jax import lax
from jax.experimental import pallas as pl
from jax.experimental.pallas import tpu as pltpu
from jax.sharding import PartitionSpec as P

SWEEPS = 4
STEP_WEIGHT = 0.5
MESH = pl.DeviceIdType.MESH

RING = 10
LAG_SUM = 3
LAG_RELAY = 7
LAG_GRAD = 8
EXTRA = 6
EXTRA_LAST = 2
FIRST_CHUNK = 7
CHUNK_TURNS = (3, 4)
GROUPS = 2


def kernel(x_hbm, y_hbm, w0_hbm, eta_hbm, lam_hbm, w_out, r_out,
           xb, sb, st, gb, gr, wb, eb, lb, rb, rt, ub, ur, fr,
           x_sem, in_sem, us_sem, ur_sem, rs_sem, rr_sem, lo_sem, gs_sem, gr_sem, ss_sem, sr_sem, wo_sem):
    problem, samp, feat = lax.axis_index("problem"), lax.axis_index("samp"), lax.axis_index("feat")
    partner = feat + 1 - 2 * lax.rem(feat, 2)
    mate = lax.rem(feat + 2, 4)
    cross = lax.rem(partner + 2, 4)
    to_partner, to_mate, to_cross = (problem, samp, partner), (problem, samp, mate), (problem, samp, cross)
    other = 1 - samp
    to_other = (problem, other, feat)

    owned = rb.shape[2]
    tile_rows = 4 * owned
    tiles = rb.shape[1]
    width = gb.shape[2]
    chunks = gr.shape[1]
    chunk = gb.shape[3]
    half_feats = chunks * chunk
    phases = GROUPS * (SWEEPS + 1)
    steps, short = tiles + EXTRA, tiles + EXTRA_LAST
    grad_end = tiles - 1 + LAG_GRAD
    total_rows = 2 * tiles * tile_rows

    def remote(src, dst, send, recv, device):
        return pltpu.make_async_remote_copy(src_ref=src, dst_ref=dst, send_sem=send, recv_sem=recv, device_id=device, device_id_type=MESH)

    barrier = pltpu.get_barrier_semaphore()
    for device in (to_partner, to_mate, to_cross, to_other):
        pl.semaphore_signal(barrier, inc=1, device_id=device, device_id_type=MESH)

    def load_tile(tile, slot):
        rows = pl.ds(pl.multiple_of(tile * tile_rows, tile_rows), tile_rows)
        return pltpu.make_async_copy(x_hbm.at[rows], xb.at[slot], x_sem.at[slot])

    own_feats = pl.ds(pl.multiple_of(samp * half_feats, half_feats), half_feats)
    other_feats = pl.ds(pl.multiple_of(other * half_feats, half_feats), half_feats)

    def own_coef(group):
        return pltpu.make_async_copy(w0_hbm.at[own_feats, pl.ds(group * width, width)], wb.at[group], in_sem.at[group])

    def other_coef(group):
        return pltpu.make_async_copy(w0_hbm.at[other_feats, pl.ds(group * width, width)], st, in_sem.at[GROUPS + group])

    def round_coef(group):
        own_coef(group).wait()
        other_coef(group).wait()
        for each in range(chunks):
            rows = pl.ds(each * chunk, chunk)
            for start, source in ((samp, wb.at[group]), (other, st)):
                target = pl.ds(pl.multiple_of(start * half_feats + each * chunk, chunk), chunk)
                sb[group, target] = source[rows].astype(jnp.bfloat16)

    rest = [
        pltpu.make_async_copy(y_hbm.at[:, feat, :, pl.ds(g * width, width)], rb.at[g], in_sem.at[2 * GROUPS + g])
        for g in range(GROUPS)
    ]
    rest.append(pltpu.make_async_copy(eta_hbm.at[pl.ds(samp * chunks, chunks)], eb, in_sem.at[3 * GROUPS]))
    rest.append(pltpu.make_async_copy(lam_hbm, lb, in_sem.at[3 * GROUPS + 1]))
    own_coef(0).start()
    other_coef(0).start()
    load_tile(0, 0).start()
    load_tile(1, 1).start()
    for copy in rest:
        copy.start()
    own_coef(1).start()
    for slot in range(2, RING):
        load_tile(slot, slot).start()
    round_coef(0)
    other_coef(1).start()
    for copy in rest:
        copy.wait()
    pl.semaphore_wait(barrier, 4)

    def product_copies(slot):
        return [
            remote(ub.at[slot, owner], ur.at[slot, rel], us_sem.at[slot], ur_sem.at[slot], device)
            for rel, (owner, device) in enumerate(((mate, to_mate), (cross, to_cross), (partner, to_partner)))
        ]

    def products(slot):
        return remote(ur.at[slot], ur.at[slot], us_sem.at[slot], ur_sem.at[slot], to_partner)

    def resid_rows(tile, owner, group):
        return r_out.at[
            pl.ds(pl.multiple_of(tile * tile_rows + owner * owned, owned), owned),
            pl.ds(pl.multiple_of(group * width, width), width),
        ]

    def resid_mate(slot):
        return remote(rt.at[slot, feat], rt.at[slot, feat], rs_sem.at[slot, 0], rr_sem.at[slot, 0], to_mate)

    def resid_partner(slot):
        return remote(rt.at[slot, feat], rt.at[slot, feat], rs_sem.at[slot, 0], rr_sem.at[slot, 1], to_partner)

    def resid_relay(slot):
        return remote(rt.at[slot, mate], rt.at[slot, mate], rs_sem.at[slot, 0], rr_sem.at[slot, 1], to_partner)

    def resid_received(slot):
        return remote(rt.at[slot, pl.ds(0, 2)], rt.at[slot, pl.ds(0, 2)], rs_sem.at[slot, 0], rr_sem.at[slot, 1], to_partner)

    def resid_sent(slot):
        return remote(rt.at[slot, pl.ds(0, 3)], rt.at[slot, pl.ds(0, 3)], rs_sem.at[slot, 0], rr_sem.at[slot, 1], to_partner)

    def last_mate(slot, group, tile):
        return remote(rb.at[group, tile], fr.at[slot], rs_sem.at[slot, 0], rr_sem.at[slot, 0], to_mate)

    def last_partner(slot, group, tile):
        return remote(rb.at[group, tile], resid_rows(tile, feat, group), rs_sem.at[slot, 1], rr_sem.at[slot, 1], to_partner)

    def last_relay(slot, group, tile):
        return remote(fr.at[slot], resid_rows(tile, mate, group), rs_sem.at[slot, 2], rr_sem.at[slot, 2], to_partner)

    def last_own(slot, group, tile):
        return pltpu.make_async_copy(rb.at[group, tile], resid_rows(tile, feat, group), lo_sem.at[slot, 0])

    def last_mates(slot, group, tile):
        return pltpu.make_async_copy(fr.at[slot], resid_rows(tile, mate, group), lo_sem.at[slot, 1])

    def grad_copy(group, index):
        return remote(gb.at[group, other * chunks + index], gr.at[group, index], gs_sem.at[group, index], gr_sem.at[group, index], to_other)

    def delta_copy(group, index, count):
        rows = pl.ds(pl.multiple_of(samp * half_feats + index * chunk, chunk), count * chunk)
        return remote(sb.at[group, rows], sb.at[group, rows], ss_sem.at[group], sr_sem.at[group], to_other)

    def coef_rows(group):
        return w_out.at[own_feats, pl.ds(group * width, width)]

    def coef_remote(group):
        return remote(wb.at[group], coef_rows(group), wo_sem.at[group, 0], wo_sem.at[group, 1], to_other)

    def coef_local(group):
        return pltpu.make_async_copy(wb.at[group], coef_rows(group), wo_sem.at[group, 2])

    def step(_, states):
        def turn_of(name):
            tile, phase, slot = states[name]
            active = (tile >= 0) & (tile < tiles) & (phase < phases)
            return active, phase >= phases - GROUPS, phase, phase & 1, tile, slot

        active_x, _, phase_x, group_x, tile_x, slot_x = turn_of("product")
        active, final, phase, group, tile, slot = turn_of("relay")
        active_s, final_s, phase_s, group_s, tile_s, slot_s = turn_of("sum")
        active_g, final_g, phase_g, group_g, tile_g, slot_g = turn_of("grad")
        turn, chunk_phase, _ = states["chunk"]
        if CHUNK_TURNS == (3, 4):
            part, index = turn & 3, 3 * lax.shift_right_logical(turn, 2) + (turn & 3)
        elif CHUNK_TURNS == (1, 2):
            part, index = turn & 1, lax.shift_right_logical(turn, 1)
        else:
            part, index = 0, turn

        @pl.when(active & jnp.logical_not(final))
        def _():
            resid_mate(slot).wait_recv()
            resid_relay(slot).start()

        @pl.when(active & final)
        def _():
            last_mate(slot, group, tile).wait_recv()
            last_relay(slot, group, tile).start()
            last_mates(slot, group, tile).start()

        @pl.when((turn >= 0) & (chunk_phase < phases - GROUPS) & (part < CHUNK_TURNS[0]) & (index < chunks))
        def _():
            group = chunk_phase & 1
            grad_copy(group, index).wait()
            summed = gb[group, samp * chunks + index] + gr[group, index]
            gradient = summed.T * (1.0 / total_rows)
            rows = pl.ds(pl.multiple_of(index * chunk, chunk), chunk)
            coef = wb[group, rows]
            rate = jnp.broadcast_to(eb[index], (width, chunk)).T
            delta = rate * (gradient - lb[group] * coef)
            wb[group, rows] = coef + STEP_WEIGHT * delta
            sb[group, pl.ds(pl.multiple_of(samp * half_feats + index * chunk, chunk), chunk)] = delta.astype(jnp.bfloat16)
            delta_copy(group, index, 1).start()

            @pl.when((chunk_phase == phases - GROUPS - 1) & (index == chunks - 1))
            def _():
                for each in range(GROUPS):
                    coef_remote(each).start()
                    coef_local(each).start()

        @pl.when(active_x & (tile_x == 0) & (phase_x >= GROUPS))
        def _():
            delta_copy(group_x, 0, chunks).wait()

        @pl.when(active_x & (tile_x == 0) & (phase_x == 1))
        def _():
            round_coef(1)

        work_g = active_g & jnp.logical_not(final_g)

        def multiply():
            delta = sb[group_x]
            product = jnp.dot(xb[slot_x], jnp.concatenate([delta, delta], axis=1), preferred_element_type=jnp.float32)
            ub[slot_x] = product[:, :width].astype(jnp.bfloat16).reshape(4, owned, width)

        def send():
            for copy in product_copies(slot_x):
                copy.start()

        def accumulate():
            left = jnp.concatenate([rt[slot_g, owner] for owner in range(4)], axis=1)
            for each in range(2 * chunks):
                share = jnp.dot(left, xb[slot_g, :, each * chunk:(each + 1) * chunk], preferred_element_type=jnp.float32)
                gb[group_g, each] = jnp.where(tile_g == 0, 0.0, gb[group_g, each]) + share

        @pl.when(active_x & work_g)
        def _():
            load_tile(tile_x, slot_x).wait()
            resid_received(slot_g).wait_recv()
            multiply()
            accumulate()
            send()

        @pl.when(active_x & jnp.logical_not(work_g))
        def _():
            load_tile(tile_x, slot_x).wait()
            multiply()
            send()

        @pl.when(jnp.logical_not(active_x) & work_g)
        def _():
            resid_received(slot_g).wait_recv()
            accumulate()

        @pl.when(work_g)
        def _():
            @pl.when(tile_g == tiles - 1)
            def _():
                for each in range(chunks):
                    grad_copy(group_g, each).start()

            resid_sent(slot_g).wait_send()

        @pl.when(active_g & final_g)
        def _():
            last_partner(slot_g, group_g, tile_g).wait()
            last_relay(slot_g, group_g, tile_g).wait()
            last_mate(slot_g, group_g, tile_g).wait_send()
            last_own(slot_g, group_g, tile_g).wait()
            last_mates(slot_g, group_g, tile_g).wait()

        @pl.when(active_g)
        def _():
            products(slot_g).wait_send()

            @pl.when(phase_g * tiles + tile_g + RING < phases * tiles)
            def _():
                ahead = jnp.where(tile_g + RING >= tiles, tile_g + RING - tiles, tile_g + RING)
                load_tile(ahead, slot_g).start()

        @pl.when(active_s)
        def _():
            products(slot_s).wait_recv()
            summed = ub[slot_s, feat].astype(jnp.float32) + ur[slot_s, 2].astype(jnp.float32)
            summed = summed + (ur[slot_s, 0].astype(jnp.float32) + ur[slot_s, 1].astype(jnp.float32))
            weight = jnp.where(phase_s < GROUPS, 1.0, STEP_WEIGHT)
            resid = rb[group_s, tile_s] - weight * summed
            rb[group_s, tile_s] = resid

            @pl.when(jnp.logical_not(final_s))
            def _():
                rt[slot_s, feat] = resid.astype(jnp.bfloat16).T
                resid_mate(slot_s).start()
                resid_partner(slot_s).start()

            @pl.when(final_s)
            def _():
                last_mate(slot_s, group_s, tile_s).start()
                last_partner(slot_s, group_s, tile_s).start()
                last_own(slot_s, group_s, tile_s).start()

        following = {}
        for name, (tile, phase, slot) in states.items():
            within = (tile >= 0) & (tile < tiles)
            slot = jnp.where(within, slot + 1, slot)
            wrap = tile == jnp.where(phase == phases - GROUPS, short - 1, steps - 1)
            following[name] = (
                jnp.where(wrap, 0, tile + 1),
                jnp.where(wrap, phase + 1, phase),
                jnp.where(slot == RING, 0, slot),
            )
        return following

    zero = jnp.int32(0)
    lags = {"product": 0, "sum": LAG_SUM, "relay": LAG_RELAY, "grad": LAG_GRAD, "chunk": grad_end + FIRST_CHUNK}
    start = {name: (jnp.int32(-lag), zero, zero) for name, lag in lags.items()}
    lax.fori_loop(0, (phases - 2) * steps + short + tiles + LAG_GRAD, step, start)
    for group in range(GROUPS):
        coef_remote(group).wait()
        coef_local(group).wait()


def sweeps(design, targets, coef_init, step_sizes, ridge_weights):
    rows, feats = design.shape
    width = targets.shape[1] // GROUPS
    owned = 128
    tiles = rows // (4 * owned)
    chunks = 8
    chunk = feats // (2 * chunks)
    dma = pltpu.SemaphoreType.DMA
    f32, bf16 = jnp.float32, jnp.bfloat16
    scratch = [
        pltpu.VMEM((RING, 4 * owned, feats), bf16),
        pltpu.VMEM((GROUPS, feats, width), bf16),
        pltpu.VMEM((feats // 2, width), f32),
        pltpu.VMEM((GROUPS, 2 * chunks, width, chunk), f32),
        pltpu.VMEM((GROUPS, chunks, width, chunk), f32),
        pltpu.VMEM((GROUPS, feats // 2, width), f32),
        pltpu.VMEM((chunks, 1, chunk), f32),
        pltpu.VMEM((GROUPS, 1, width), f32),
        pltpu.VMEM((GROUPS, tiles, owned, width), f32),
        pltpu.VMEM((RING, 4, width, owned), bf16),
        pltpu.VMEM((RING, 4, owned, width), bf16),
        pltpu.VMEM((RING, 3, owned, width), bf16),
        pltpu.VMEM((RING, owned, width), f32),
        dma((RING,)),
        dma((3 * GROUPS + 2,)),
        dma((RING,)),
        dma((RING,)),
        dma((RING, 3)),
        dma((RING, 3)),
        dma((RING, 2)),
        dma((GROUPS, chunks)),
        dma((GROUPS, chunks)),
        dma((GROUPS,)),
        dma((GROUPS,)),
        dma((GROUPS, 3)),
    ]
    return pl.pallas_call(
        kernel,
        out_shape=(jax.ShapeDtypeStruct(coef_init.shape, f32), jax.ShapeDtypeStruct(targets.shape, f32)),
        in_specs=[pl.BlockSpec(memory_space=pl.ANY)] * 5,
        out_specs=[pl.BlockSpec(memory_space=pl.ANY)] * 2,
        scratch_shapes=scratch,
        compiler_params=pltpu.CompilerParams(collective_id=0, has_side_effects=True, vmem_limit_bytes=63 * 2**20),
    )(
        design,
        targets.reshape(tiles, 4, owned, targets.shape[1]),
        coef_init,
        step_sizes.reshape(2 * chunks, 1, chunk),
        ridge_weights.reshape(GROUPS, 1, width),
    )


def solution(mesh):
    design_spec = P(("problem", "samp"), "feat")
    rows_spec = P(("problem", "samp"), None)
    coef_spec = P(("problem", "feat"), None)
    step_spec = P(("problem", "feat"))
    ridge_spec = P("problem")
    return jax.shard_map(sweeps, mesh=mesh, in_specs=(design_spec, rows_spec, coef_spec, step_spec, ridge_spec), out_specs=(coef_spec, rows_spec), check_vma=False)
```

```python
import functools

import jax
import jax.numpy as jnp
from jax import lax
from jax.experimental import pallas as pl
from jax.experimental.pallas import tpu as pltpu
from jax.sharding import PartitionSpec as P

SWEEPS = 4
STEP_WEIGHT = 0.5
MESH = pl.DeviceIdType.MESH

RING = 10
LAG_SUM = 3
LAG_RELAY = 7
LAG_GRAD = 8
EXTRA = 6
EXTRA_LAST = 2
FIRST_CHUNK = 7
CHUNK_TURNS = (3, 4)
GROUPS = 2


def kernel(x_hbm, y_hbm, w0_hbm, eta_hbm, lam_hbm, w_out, r_out,
           xb, sb, gb, gr, eb, lb, rt, ub, ur,
           x_sem, in_sem, us_sem, ur_sem, rs_sem, rr_sem, gs_sem, gr_sem, ss_sem, sr_sem, wo_sem):
    problem, samp, feat = lax.axis_index("problem"), lax.axis_index("samp"), lax.axis_index("feat")
    partner = feat + 1 - 2 * lax.rem(feat, 2)
    mate = lax.rem(feat + 2, 4)
    cross = lax.rem(partner + 2, 4)
    to_partner, to_mate, to_cross = (problem, samp, partner), (problem, samp, mate), (problem, samp, cross)
    other = 1 - samp
    to_other = (problem, other, feat)

    owned = r_out.shape[2]
    tile_rows = 4 * owned
    tiles = r_out.shape[0]
    width = gb.shape[2]
    chunks = gr.shape[1]
    chunk = gb.shape[3]
    half_feats = chunks * chunk
    phases = GROUPS * (SWEEPS + 1)
    steps, short = tiles + EXTRA, tiles + EXTRA_LAST
    grad_end = tiles - 1 + LAG_GRAD
    total_rows = 2 * tiles * tile_rows

    def remote(src, dst, send, recv, device):
        return pltpu.make_async_remote_copy(src_ref=src, dst_ref=dst, send_sem=send, recv_sem=recv, device_id=device, device_id_type=MESH)

    barrier = pltpu.get_barrier_semaphore()
    for device in (to_partner, to_mate, to_cross, to_other):
        pl.semaphore_signal(barrier, inc=1, device_id=device, device_id_type=MESH)

    def load_tile(tile, slot):
        rows = pl.ds(pl.multiple_of(tile * tile_rows, tile_rows), tile_rows)
        return pltpu.make_async_copy(x_hbm.at[rows], xb.at[slot], x_sem.at[slot])

    own_feats = pl.ds(pl.multiple_of(samp * half_feats, half_feats), half_feats)
    other_feats = pl.ds(pl.multiple_of(other * half_feats, half_feats), half_feats)

    def targets_of(group):
        return pl.ds(pl.multiple_of(group * width, width), width)

    def first_coef(group):
        return pltpu.make_async_copy(w0_hbm.at[:, targets_of(group)], w_out.at[:, targets_of(group)], in_sem.at[group])

    def round_coef(group):
        first_coef(group).wait()
        for each in range(2 * chunks):
            rows = pl.ds(each * chunk, chunk)
            sb[group, rows] = w_out[rows, group * width:(group + 1) * width].astype(jnp.bfloat16)

    rest = [
        pltpu.make_async_copy(y_hbm.at[:, feat], r_out.at[:, feat], in_sem.at[GROUPS]),
        pltpu.make_async_copy(eta_hbm.at[pl.ds(samp * chunks, chunks)], eb, in_sem.at[GROUPS + 1]),
        pltpu.make_async_copy(lam_hbm, lb, in_sem.at[GROUPS + 2]),
    ]
    first_coef(0).start()
    load_tile(0, 0).start()
    load_tile(1, 1).start()
    for copy in rest:
        copy.start()
    first_coef(1).start()
    for slot in range(2, RING):
        load_tile(slot, slot).start()
    round_coef(0)
    for copy in rest:
        copy.wait()
    pl.semaphore_wait(barrier, 4)

    def product_copies(slot):
        return [
            remote(ub.at[slot, owner], ur.at[slot, rel], us_sem.at[slot], ur_sem.at[slot], device)
            for rel, (owner, device) in enumerate(((mate, to_mate), (cross, to_cross), (partner, to_partner)))
        ]

    def products(slot):
        return remote(ur.at[slot], ur.at[slot], us_sem.at[slot], ur_sem.at[slot], to_partner)

    def resid_mate(slot):
        return remote(rt.at[slot, feat], rt.at[slot, feat], rs_sem.at[slot, 0], rr_sem.at[slot, 0], to_mate)

    def resid_partner(slot):
        return remote(rt.at[slot, feat], rt.at[slot, feat], rs_sem.at[slot, 0], rr_sem.at[slot, 1], to_partner)

    def resid_relay(slot):
        return remote(rt.at[slot, mate], rt.at[slot, mate], rs_sem.at[slot, 0], rr_sem.at[slot, 1], to_partner)

    def resid_received(slot):
        return remote(rt.at[slot, pl.ds(0, 2)], rt.at[slot, pl.ds(0, 2)], rs_sem.at[slot, 0], rr_sem.at[slot, 1], to_partner)

    def resid_sent(slot):
        return remote(rt.at[slot, pl.ds(0, 3)], rt.at[slot, pl.ds(0, 3)], rs_sem.at[slot, 0], rr_sem.at[slot, 1], to_partner)

    def last_rows(tile, owner, group):
        return r_out.at[tile, owner, :, targets_of(group)]

    def last_mate(slot, group, tile):
        rows = last_rows(tile, feat, group)
        return remote(rows, rows, rs_sem.at[slot, 0], rr_sem.at[slot, 0], to_mate)

    def last_partner(slot, group, tile):
        rows = last_rows(tile, feat, group)
        return remote(rows, rows, rs_sem.at[slot, 1], rr_sem.at[slot, 1], to_partner)

    def last_relay(slot, group, tile):
        rows = last_rows(tile, mate, group)
        return remote(rows, rows, rs_sem.at[slot, 2], rr_sem.at[slot, 2], to_partner)

    def grad_copy(group, index):
        return remote(gb.at[group, other * chunks + index], gr.at[group, index], gs_sem.at[group, index], gr_sem.at[group, index], to_other)

    def delta_copy(group, index, count):
        rows = pl.ds(pl.multiple_of(samp * half_feats + index * chunk, chunk), count * chunk)
        return remote(sb.at[group, rows], sb.at[group, rows], ss_sem.at[group], sr_sem.at[group], to_other)

    def coef_copy(group):
        rows = w_out.at[own_feats, targets_of(group)]
        return remote(rows, rows, wo_sem.at[group, 0], wo_sem.at[group, 1], to_other)

    def step(_, states):
        def turn_of(name):
            tile, phase, slot = states[name]
            active = (tile >= 0) & (tile < tiles) & (phase < phases)
            return active, phase >= phases - GROUPS, phase, phase & 1, tile, slot

        active_x, _, phase_x, group_x, tile_x, slot_x = turn_of("product")
        active, final, phase, group, tile, slot = turn_of("relay")
        active_s, final_s, phase_s, group_s, tile_s, slot_s = turn_of("sum")
        active_g, final_g, phase_g, group_g, tile_g, slot_g = turn_of("grad")
        turn, chunk_phase, _ = states["chunk"]
        if CHUNK_TURNS == (3, 4):
            part, index = turn & 3, 3 * lax.shift_right_logical(turn, 2) + (turn & 3)
        elif CHUNK_TURNS == (1, 2):
            part, index = turn & 1, lax.shift_right_logical(turn, 1)
        else:
            part, index = 0, turn

        @pl.when(active & jnp.logical_not(final))
        def _():
            resid_mate(slot).wait_recv()
            resid_relay(slot).start()

        @pl.when(active & final)
        def _():
            last_mate(slot, group, tile).wait_recv()
            last_relay(slot, group, tile).start()

        @pl.when((turn >= 0) & (chunk_phase < phases - GROUPS) & (part < CHUNK_TURNS[0]) & (index < chunks))
        def _():
            group = chunk_phase & 1
            grad_copy(group, index).wait()
            summed = gb[group, samp * chunks + index] + gr[group, index]
            gradient = summed.T * (1.0 / total_rows)
            rows = pl.ds(pl.multiple_of(samp * half_feats + index * chunk, chunk), chunk)
            coef = w_out[rows, targets_of(group)]
            rate = jnp.broadcast_to(eb[index], (width, chunk)).T
            delta = rate * (gradient - lb[group] * coef)
            w_out[rows, targets_of(group)] = coef + STEP_WEIGHT * delta
            sb[group, rows] = delta.astype(jnp.bfloat16)
            delta_copy(group, index, 1).start()

            @pl.when((chunk_phase == phases - GROUPS - 1) & (index == chunks - 1))
            def _():
                for each in range(GROUPS):
                    coef_copy(each).start()

        @pl.when(active_x & (tile_x == 0) & (phase_x >= GROUPS))
        def _():
            delta_copy(group_x, 0, chunks).wait()

        @pl.when(active_x & (tile_x == 0) & (phase_x == 1))
        def _():
            round_coef(1)

        work_g = active_g & jnp.logical_not(final_g)

        def multiply():
            delta = sb[group_x]
            product = jnp.dot(xb[slot_x], jnp.concatenate([delta, delta], axis=1), preferred_element_type=jnp.float32)
            ub[slot_x] = product[:, :width].astype(jnp.bfloat16).reshape(4, owned, width)

        def send():
            for copy in product_copies(slot_x):
                copy.start()

        def accumulate():
            left = jnp.concatenate([rt[slot_g, owner] for owner in range(4)], axis=1)
            for each in range(2 * chunks):
                share = jnp.dot(left, xb[slot_g, :, each * chunk:(each + 1) * chunk], preferred_element_type=jnp.float32)
                gb[group_g, each] = jnp.where(tile_g == 0, 0.0, gb[group_g, each]) + share

        @pl.when(active_x & work_g)
        def _():
            load_tile(tile_x, slot_x).wait()
            resid_received(slot_g).wait_recv()
            multiply()
            accumulate()
            send()

        @pl.when(active_x & jnp.logical_not(work_g))
        def _():
            load_tile(tile_x, slot_x).wait()
            multiply()
            send()

        @pl.when(jnp.logical_not(active_x) & work_g)
        def _():
            resid_received(slot_g).wait_recv()
            accumulate()

        @pl.when(work_g)
        def _():
            @pl.when(tile_g == tiles - 1)
            def _():
                for each in range(chunks):
                    grad_copy(group_g, each).start()

            resid_sent(slot_g).wait_send()

        @pl.when(active_g & final_g)
        def _():
            last_partner(slot_g, group_g, tile_g).wait()
            last_relay(slot_g, group_g, tile_g).wait()
            last_mate(slot_g, group_g, tile_g).wait_send()

        @pl.when(active_g)
        def _():
            products(slot_g).wait_send()

            @pl.when(phase_g * tiles + tile_g + RING < phases * tiles)
            def _():
                ahead = jnp.where(tile_g + RING >= tiles, tile_g + RING - tiles, tile_g + RING)
                load_tile(ahead, slot_g).start()

        @pl.when(active_s)
        def _():
            products(slot_s).wait_recv()
            summed = ub[slot_s, feat].astype(jnp.float32) + ur[slot_s, 2].astype(jnp.float32)
            summed = summed + (ur[slot_s, 0].astype(jnp.float32) + ur[slot_s, 1].astype(jnp.float32))
            weight = jnp.where(phase_s < GROUPS, 1.0, STEP_WEIGHT)
            resid = r_out[tile_s, feat, :, targets_of(group_s)] - weight * summed
            r_out[tile_s, feat, :, targets_of(group_s)] = resid

            @pl.when(jnp.logical_not(final_s))
            def _():
                rt[slot_s, feat] = resid.astype(jnp.bfloat16).T
                resid_mate(slot_s).start()
                resid_partner(slot_s).start()

            @pl.when(final_s)
            def _():
                last_mate(slot_s, group_s, tile_s).start()
                last_partner(slot_s, group_s, tile_s).start()

        following = {}
        for name, (tile, phase, slot) in states.items():
            within = (tile >= 0) & (tile < tiles)
            slot = jnp.where(within, slot + 1, slot)
            wrap = tile == jnp.where(phase == phases - GROUPS, short - 1, steps - 1)
            following[name] = (
                jnp.where(wrap, 0, tile + 1),
                jnp.where(wrap, phase + 1, phase),
                jnp.where(slot == RING, 0, slot),
            )
        return following

    zero = jnp.int32(0)
    lags = {"product": 0, "sum": LAG_SUM, "relay": LAG_RELAY, "grad": LAG_GRAD, "chunk": grad_end + FIRST_CHUNK}
    start = {name: (jnp.int32(-lag), zero, zero) for name, lag in lags.items()}
    lax.fori_loop(0, (phases - 2) * steps + short + tiles + LAG_GRAD, step, start)
    for group in range(GROUPS):
        coef_copy(group).wait()


def sweeps(design, targets, coef_init, step_sizes, ridge_weights):
    rows, feats = design.shape
    width = targets.shape[1] // GROUPS
    owned = 128
    tiles = rows // (4 * owned)
    chunks = 8
    chunk = feats // (2 * chunks)
    dma = pltpu.SemaphoreType.DMA
    f32, bf16 = jnp.float32, jnp.bfloat16
    scratch = [
        pltpu.VMEM((RING, 4 * owned, feats), bf16),
        pltpu.VMEM((GROUPS, feats, width), bf16),
        pltpu.VMEM((GROUPS, 2 * chunks, width, chunk), f32),
        pltpu.VMEM((GROUPS, chunks, width, chunk), f32),
        pltpu.VMEM((chunks, 1, chunk), f32),
        pltpu.VMEM((GROUPS, 1, width), f32),
        pltpu.VMEM((RING, 4, width, owned), bf16),
        pltpu.VMEM((RING, 4, owned, width), bf16),
        pltpu.VMEM((RING, 3, owned, width), bf16),
        dma((RING,)),
        dma((GROUPS + 3,)),
        dma((RING,)),
        dma((RING,)),
        dma((RING, 3)),
        dma((RING, 3)),
        dma((GROUPS, chunks)),
        dma((GROUPS, chunks)),
        dma((GROUPS,)),
        dma((GROUPS,)),
        dma((GROUPS, 2)),
    ]
    tiled = (tiles, 4, owned, targets.shape[1])
    coef, resid = pl.pallas_call(
        kernel,
        out_shape=(pltpu.VMEM(coef_init.shape, f32), pltpu.VMEM(tiled, f32)),
        in_specs=[pl.BlockSpec(memory_space=pl.ANY)] * 5,
        out_specs=[pl.BlockSpec(memory_space=pltpu.VMEM)] * 2,
        scratch_shapes=scratch,
        compiler_params=pltpu.CompilerParams(collective_id=0, has_side_effects=True, vmem_limit_bytes=519 * 2**20 // 10),
    )(
        design,
        targets.reshape(tiled),
        coef_init,
        step_sizes.reshape(2 * chunks, 1, chunk),
        ridge_weights.reshape(GROUPS, 1, width),
    )
    return coef, resid.reshape(targets.shape)


def solution(mesh):
    design_spec = P(("problem", "samp"), "feat")
    rows_spec = P(("problem", "samp"), None)
    coef_spec = P(("problem", "feat"), None)
    step_spec = P(("problem", "feat"))
    ridge_spec = P("problem")
    return jax.shard_map(sweeps, mesh=mesh, in_specs=(design_spec, rows_spec, coef_spec, step_spec, ridge_spec), out_specs=(coef_spec, rows_spec), check_vma=False)
```

```python
import functools

import jax
import jax.numpy as jnp
from jax import lax
from jax.experimental import pallas as pl
from jax.experimental.pallas import tpu as pltpu
from jax.sharding import PartitionSpec as P

SWEEPS = 4
STEP_WEIGHT = 0.5
MESH = pl.DeviceIdType.MESH

RING = 10
AHEAD = 2
LAG_SUM = 3
LAG_RELAY = 7
LAG_GRAD = 8
EXTRA = 6
EXTRA_LAST = 2
FIRST_CHUNK = 7
CHUNK_TURNS = (3, 4)
GROUPS = 2


def kernel(x_hbm, y_hbm, w0_hbm, eta_hbm, lam_hbm, w_out, r_out,
           xb, sb, gb, gr, eb, lb, rt, ub, ur,
           x_sem, in_sem, us_sem, ur_sem, rs_sem, rr_sem, gs_sem, gr_sem, ss_sem, sr_sem, wo_sem):
    problem, samp, feat = lax.axis_index("problem"), lax.axis_index("samp"), lax.axis_index("feat")
    partner = feat + 1 - 2 * lax.rem(feat, 2)
    mate = lax.rem(feat + 2, 4)
    cross = lax.rem(partner + 2, 4)
    to_partner, to_mate, to_cross = (problem, samp, partner), (problem, samp, mate), (problem, samp, cross)
    other = 1 - samp
    to_other = (problem, other, feat)

    owned = r_out.shape[2]
    tile_rows = 4 * owned
    tiles = r_out.shape[0]
    width = gb.shape[2]
    chunks = gr.shape[1]
    chunk = gb.shape[3]
    half_feats = chunks * chunk
    phases = GROUPS * (SWEEPS + 1)
    steps, short = tiles + EXTRA, tiles + EXTRA_LAST
    grad_end = tiles - 1 + LAG_GRAD
    total_rows = 2 * tiles * tile_rows

    def remote(src, dst, send, recv, device):
        return pltpu.make_async_remote_copy(src_ref=src, dst_ref=dst, send_sem=send, recv_sem=recv, device_id=device, device_id_type=MESH)

    barrier = pltpu.get_barrier_semaphore()
    for device in (to_partner, to_mate, to_cross, to_other):
        pl.semaphore_signal(barrier, inc=1, device_id=device, device_id_type=MESH)

    def load_tile(tile, slot):
        rows = pl.ds(pl.multiple_of(tile * tile_rows, tile_rows), tile_rows)
        return pltpu.make_async_copy(x_hbm.at[rows], xb.at[slot], x_sem.at[slot])

    own_feats = pl.ds(pl.multiple_of(samp * half_feats, half_feats), half_feats)
    other_feats = pl.ds(pl.multiple_of(other * half_feats, half_feats), half_feats)

    def targets_of(group):
        return pl.ds(pl.multiple_of(group * width, width), width)

    def first_coef(group):
        return pltpu.make_async_copy(w0_hbm.at[:, targets_of(group)], w_out.at[:, targets_of(group)], in_sem.at[group])

    def round_coef(group):
        first_coef(group).wait()
        for each in range(2 * chunks):
            rows = pl.ds(each * chunk, chunk)
            sb[group, rows] = w_out[rows, group * width:(group + 1) * width].astype(jnp.bfloat16)

    rest = [
        pltpu.make_async_copy(y_hbm.at[:, feat], r_out.at[:, feat], in_sem.at[GROUPS]),
        pltpu.make_async_copy(eta_hbm.at[pl.ds(samp * chunks, chunks)], eb, in_sem.at[GROUPS + 1]),
        pltpu.make_async_copy(lam_hbm, lb, in_sem.at[GROUPS + 2]),
    ]
    first_coef(0).start()
    load_tile(0, 0).start()
    for copy in rest:
        copy.start()
    for slot in range(1, AHEAD):
        load_tile(slot, slot).start()
    round_coef(0)
    pl.semaphore_wait(barrier, 4)

    def product_copies(slot):
        return [
            remote(ub.at[slot, owner], ur.at[slot, rel], us_sem.at[slot], ur_sem.at[slot], device)
            for rel, (owner, device) in enumerate(((mate, to_mate), (cross, to_cross), (partner, to_partner)))
        ]

    def products(slot):
        return remote(ur.at[slot], ur.at[slot], us_sem.at[slot], ur_sem.at[slot], to_partner)

    def resid_mate(slot):
        return remote(rt.at[slot, feat], rt.at[slot, feat], rs_sem.at[slot, 0], rr_sem.at[slot, 0], to_mate)

    def resid_partner(slot):
        return remote(rt.at[slot, feat], rt.at[slot, feat], rs_sem.at[slot, 0], rr_sem.at[slot, 1], to_partner)

    def resid_relay(slot):
        return remote(rt.at[slot, mate], rt.at[slot, mate], rs_sem.at[slot, 0], rr_sem.at[slot, 1], to_partner)

    def resid_received(slot):
        return remote(rt.at[slot, pl.ds(0, 2)], rt.at[slot, pl.ds(0, 2)], rs_sem.at[slot, 0], rr_sem.at[slot, 1], to_partner)

    def resid_sent(slot):
        return remote(rt.at[slot, pl.ds(0, 3)], rt.at[slot, pl.ds(0, 3)], rs_sem.at[slot, 0], rr_sem.at[slot, 1], to_partner)

    def last_rows(tile, owner, group):
        return r_out.at[tile, owner, :, targets_of(group)]

    def last_mate(slot, group, tile):
        rows = last_rows(tile, feat, group)
        return remote(rows, rows, rs_sem.at[slot, 0], rr_sem.at[slot, 0], to_mate)

    def last_partner(slot, group, tile):
        rows = last_rows(tile, feat, group)
        return remote(rows, rows, rs_sem.at[slot, 1], rr_sem.at[slot, 1], to_partner)

    def last_relay(slot, group, tile):
        rows = last_rows(tile, mate, group)
        return remote(rows, rows, rs_sem.at[slot, 2], rr_sem.at[slot, 2], to_partner)

    def grad_copy(group, index):
        return remote(gb.at[group, other * chunks + index], gr.at[group, index], gs_sem.at[group, index], gr_sem.at[group, index], to_other)

    def delta_copy(group, index, count):
        rows = pl.ds(pl.multiple_of(samp * half_feats + index * chunk, chunk), count * chunk)
        return remote(sb.at[group, rows], sb.at[group, rows], ss_sem.at[group], sr_sem.at[group], to_other)

    def coef_copy(group):
        rows = w_out.at[own_feats, targets_of(group)]
        return remote(rows, rows, wo_sem.at[group, 0], wo_sem.at[group, 1], to_other)

    def step(_, states):
        def turn_of(name):
            tile, phase, slot = states[name]
            active = (tile >= 0) & (tile < tiles) & (phase < phases)
            return active, phase >= phases - GROUPS, phase, phase & 1, tile, slot

        active_x, _, phase_x, group_x, tile_x, slot_x = turn_of("product")
        active, final, phase, group, tile, slot = turn_of("relay")
        active_s, final_s, phase_s, group_s, tile_s, slot_s = turn_of("sum")
        active_g, final_g, phase_g, group_g, tile_g, slot_g = turn_of("grad")
        turn, chunk_phase, _ = states["chunk"]
        if CHUNK_TURNS == (3, 4):
            part, index = turn & 3, 3 * lax.shift_right_logical(turn, 2) + (turn & 3)
        elif CHUNK_TURNS == (1, 2):
            part, index = turn & 1, lax.shift_right_logical(turn, 1)
        else:
            part, index = 0, turn

        @pl.when(active & jnp.logical_not(final))
        def _():
            resid_mate(slot).wait_recv()
            resid_relay(slot).start()

        @pl.when(active & final)
        def _():
            last_mate(slot, group, tile).wait_recv()
            last_relay(slot, group, tile).start()

        @pl.when((turn >= 0) & (chunk_phase < phases - GROUPS) & (part < CHUNK_TURNS[0]) & (index < chunks))
        def _():
            group = chunk_phase & 1
            grad_copy(group, index).wait()
            summed = gb[group, samp * chunks + index] + gr[group, index]
            gradient = summed.T * (1.0 / total_rows)
            rows = pl.ds(pl.multiple_of(samp * half_feats + index * chunk, chunk), chunk)
            coef = w_out[rows, targets_of(group)]
            rate = jnp.broadcast_to(eb[index], (width, chunk)).T
            delta = rate * (gradient - lb[group] * coef)
            w_out[rows, targets_of(group)] = coef + STEP_WEIGHT * delta
            sb[group, rows] = delta.astype(jnp.bfloat16)
            delta_copy(group, index, 1).start()

            @pl.when((chunk_phase == phases - GROUPS - 1) & (index == chunks - 1))
            def _():
                for each in range(GROUPS):
                    coef_copy(each).start()

        @pl.when(active_x & (tile_x == 0) & (phase_x >= GROUPS))
        def _():
            delta_copy(group_x, 0, chunks).wait()

        @pl.when(active_x & (tile_x == 0) & (phase_x == 1))
        def _():
            round_coef(1)

        @pl.when(active_x & (phase_x == 0))
        def _():
            @pl.when(tile_x < RING - AHEAD)
            def _():
                load_tile(tile_x + AHEAD, slot_x + AHEAD).start()

            @pl.when(tile_x == RING - AHEAD)
            def _():
                first_coef(1).start()

        work_g = active_g & jnp.logical_not(final_g)

        def multiply():
            delta = sb[group_x]
            product = jnp.dot(xb[slot_x], jnp.concatenate([delta, delta], axis=1), preferred_element_type=jnp.float32)
            ub[slot_x] = product[:, :width].astype(jnp.bfloat16).reshape(4, owned, width)

        def send():
            for copy in product_copies(slot_x):
                copy.start()

        def accumulate():
            left = jnp.concatenate([rt[slot_g, owner] for owner in range(4)], axis=1)
            for each in range(2 * chunks):
                share = jnp.dot(left, xb[slot_g, :, each * chunk:(each + 1) * chunk], preferred_element_type=jnp.float32)
                gb[group_g, each] = jnp.where(tile_g == 0, 0.0, gb[group_g, each]) + share

        @pl.when(active_x & work_g)
        def _():
            load_tile(tile_x, slot_x).wait()
            resid_received(slot_g).wait_recv()
            multiply()
            accumulate()
            send()

        @pl.when(active_x & jnp.logical_not(work_g))
        def _():
            load_tile(tile_x, slot_x).wait()
            multiply()
            send()

        @pl.when(jnp.logical_not(active_x) & work_g)
        def _():
            resid_received(slot_g).wait_recv()
            accumulate()

        @pl.when(work_g)
        def _():
            @pl.when(tile_g == tiles - 1)
            def _():
                for each in range(chunks):
                    grad_copy(group_g, each).start()

            resid_sent(slot_g).wait_send()

        @pl.when(active_g & final_g)
        def _():
            last_partner(slot_g, group_g, tile_g).wait()
            last_relay(slot_g, group_g, tile_g).wait()
            last_mate(slot_g, group_g, tile_g).wait_send()

        @pl.when(active_g)
        def _():
            products(slot_g).wait_send()

            @pl.when(phase_g * tiles + tile_g + RING < phases * tiles)
            def _():
                ahead = jnp.where(tile_g + RING >= tiles, tile_g + RING - tiles, tile_g + RING)
                load_tile(ahead, slot_g).start()

        @pl.when(active_s & (tile_s == 0) & (phase_s == 0))
        def _():
            for copy in rest:
                copy.wait()

        @pl.when(active_s)
        def _():
            products(slot_s).wait_recv()
            summed = ub[slot_s, feat].astype(jnp.float32) + ur[slot_s, 2].astype(jnp.float32)
            summed = summed + (ur[slot_s, 0].astype(jnp.float32) + ur[slot_s, 1].astype(jnp.float32))
            weight = jnp.where(phase_s < GROUPS, 1.0, STEP_WEIGHT)
            resid = r_out[tile_s, feat, :, targets_of(group_s)] - weight * summed
            r_out[tile_s, feat, :, targets_of(group_s)] = resid

            @pl.when(jnp.logical_not(final_s))
            def _():
                rt[slot_s, feat] = resid.astype(jnp.bfloat16).T
                resid_mate(slot_s).start()
                resid_partner(slot_s).start()

            @pl.when(final_s)
            def _():
                last_mate(slot_s, group_s, tile_s).start()
                last_partner(slot_s, group_s, tile_s).start()

        following = {}
        for name, (tile, phase, slot) in states.items():
            within = (tile >= 0) & (tile < tiles)
            slot = jnp.where(within, slot + 1, slot)
            wrap = tile == jnp.where(phase == phases - GROUPS, short - 1, steps - 1)
            following[name] = (
                jnp.where(wrap, 0, tile + 1),
                jnp.where(wrap, phase + 1, phase),
                jnp.where(slot == RING, 0, slot),
            )
        return following

    zero = jnp.int32(0)
    lags = {"product": 0, "sum": LAG_SUM, "relay": LAG_RELAY, "grad": LAG_GRAD, "chunk": grad_end + FIRST_CHUNK}
    start = {name: (jnp.int32(-lag), zero, zero) for name, lag in lags.items()}
    lax.fori_loop(0, (phases - 2) * steps + short + tiles + LAG_GRAD, step, start)
    for group in range(GROUPS):
        coef_copy(group).wait()


def sweeps(design, targets, coef_init, step_sizes, ridge_weights):
    rows, feats = design.shape
    width = targets.shape[1] // GROUPS
    owned = 128
    tiles = rows // (4 * owned)
    chunks = 8
    chunk = feats // (2 * chunks)
    dma = pltpu.SemaphoreType.DMA
    f32, bf16 = jnp.float32, jnp.bfloat16
    scratch = [
        pltpu.VMEM((RING, 4 * owned, feats), bf16),
        pltpu.VMEM((GROUPS, feats, width), bf16),
        pltpu.VMEM((GROUPS, 2 * chunks, width, chunk), f32),
        pltpu.VMEM((GROUPS, chunks, width, chunk), f32),
        pltpu.VMEM((chunks, 1, chunk), f32),
        pltpu.VMEM((GROUPS, 1, width), f32),
        pltpu.VMEM((RING, 4, width, owned), bf16),
        pltpu.VMEM((RING, 4, owned, width), bf16),
        pltpu.VMEM((RING, 3, owned, width), bf16),
        dma((RING,)),
        dma((GROUPS + 3,)),
        dma((RING,)),
        dma((RING,)),
        dma((RING, 3)),
        dma((RING, 3)),
        dma((GROUPS, chunks)),
        dma((GROUPS, chunks)),
        dma((GROUPS,)),
        dma((GROUPS,)),
        dma((GROUPS, 2)),
    ]
    tiled = (tiles, 4, owned, targets.shape[1])
    coef, resid = pl.pallas_call(
        kernel,
        out_shape=(pltpu.VMEM(coef_init.shape, f32), pltpu.VMEM(tiled, f32)),
        in_specs=[pl.BlockSpec(memory_space=pl.ANY)] * 5,
        out_specs=[pl.BlockSpec(memory_space=pltpu.VMEM)] * 2,
        scratch_shapes=scratch,
        compiler_params=pltpu.CompilerParams(collective_id=0, has_side_effects=True, vmem_limit_bytes=519 * 2**20 // 10),
    )(
        design,
        targets.reshape(tiled),
        coef_init,
        step_sizes.reshape(2 * chunks, 1, chunk),
        ridge_weights.reshape(GROUPS, 1, width),
    )
    return coef, resid.reshape(targets.shape)


def solution(mesh):
    design_spec = P(("problem", "samp"), "feat")
    rows_spec = P(("problem", "samp"), None)
    coef_spec = P(("problem", "feat"), None)
    step_spec = P(("problem", "feat"))
    ridge_spec = P("problem")
    return jax.shard_map(sweeps, mesh=mesh, in_specs=(design_spec, rows_spec, coef_spec, step_spec, ridge_spec), out_specs=(coef_spec, rows_spec), check_vma=False)
```

```python
import functools

import jax
import jax.numpy as jnp
from jax import lax
from jax.experimental import pallas as pl
from jax.experimental.pallas import tpu as pltpu
from jax.sharding import PartitionSpec as P

SWEEPS = 4
STEP_WEIGHT = 0.5
MESH = pl.DeviceIdType.MESH

RING = 10
AHEAD = 2
LAG_SUM = 3
LAG_RELAY = 7
LAG_GRAD = 8
EXTRA = 6
EXTRA_LAST = 2
FIRST_CHUNK = 7
CHUNK_TURNS = (3, 4)
GROUPS = 2


def kernel(x_hbm, y_hbm, w0_hbm, eta_hbm, lam_hbm, w_out, r_out,
           xb, sb, gb, gr, eb, lb, rt, ub, ur,
           x_sem, in_sem, us_sem, ur_sem, rs_sem, rr_sem, gs_sem, gr_sem, ss_sem, sr_sem, wo_sem):
    problem, samp, feat = lax.axis_index("problem"), lax.axis_index("samp"), lax.axis_index("feat")
    partner = feat + 1 - 2 * lax.rem(feat, 2)
    mate = lax.rem(feat + 2, 4)
    cross = lax.rem(partner + 2, 4)
    to_partner, to_mate, to_cross = (problem, samp, partner), (problem, samp, mate), (problem, samp, cross)
    other = 1 - samp
    to_other = (problem, other, feat)

    owned = r_out.shape[2]
    tile_rows = 4 * owned
    tiles = r_out.shape[0]
    width = gb.shape[2]
    chunks = gr.shape[1]
    chunk = gb.shape[3]
    half_feats = chunks * chunk
    phases = GROUPS * (SWEEPS + 1)
    steps, short = tiles + EXTRA, tiles + EXTRA_LAST
    grad_end = tiles - 1 + LAG_GRAD
    total_rows = 2 * tiles * tile_rows

    def remote(src, dst, send, recv, device):
        return pltpu.make_async_remote_copy(src_ref=src, dst_ref=dst, send_sem=send, recv_sem=recv, device_id=device, device_id_type=MESH)

    barrier = pltpu.get_barrier_semaphore()
    for device in (to_partner, to_mate, to_cross, to_other):
        pl.semaphore_signal(barrier, inc=1, device_id=device, device_id_type=MESH)

    def load_tile(tile, slot):
        rows = pl.ds(pl.multiple_of(tile * tile_rows, tile_rows), tile_rows)
        return pltpu.make_async_copy(x_hbm.at[rows], xb.at[slot], x_sem.at[slot])

    own_feats = pl.ds(pl.multiple_of(samp * half_feats, half_feats), half_feats)
    other_feats = pl.ds(pl.multiple_of(other * half_feats, half_feats), half_feats)

    def targets_of(group):
        return pl.ds(pl.multiple_of(group * width, width), width)

    def first_coef(group):
        return pltpu.make_async_copy(w0_hbm.at[:, targets_of(group)], w_out.at[:, targets_of(group)], in_sem.at[group])

    def round_coef(group):
        first_coef(group).wait()
        for each in range(2 * chunks):
            rows = pl.ds(each * chunk, chunk)
            sb[group, rows] = w_out[rows, group * width:(group + 1) * width].astype(jnp.bfloat16)

    rest = [
        pltpu.make_async_copy(y_hbm.at[:, feat], r_out.at[:, feat], in_sem.at[GROUPS]),
        pltpu.make_async_copy(eta_hbm.at[pl.ds(samp * chunks, chunks)], eb, in_sem.at[GROUPS + 1]),
        pltpu.make_async_copy(lam_hbm, lb, in_sem.at[GROUPS + 2]),
    ]
    first_coef(0).start()
    load_tile(0, 0).start()
    for copy in rest:
        copy.start()
    for slot in range(1, AHEAD):
        load_tile(slot, slot).start()
    round_coef(0)
    pl.semaphore_wait(barrier, 4)

    def product_copies(slot):
        return [
            remote(ub.at[slot, owner], ur.at[slot, rel], us_sem.at[slot], ur_sem.at[slot], device)
            for rel, (owner, device) in enumerate(((mate, to_mate), (cross, to_cross), (partner, to_partner)))
        ]

    def products(slot):
        return remote(ur.at[slot], ur.at[slot], us_sem.at[slot], ur_sem.at[slot], to_partner)

    def resid_mate(slot):
        return remote(rt.at[slot, feat], rt.at[slot, feat], rs_sem.at[slot, 0], rr_sem.at[slot, 0], to_mate)

    def resid_partner(slot):
        return remote(rt.at[slot, feat], rt.at[slot, feat], rs_sem.at[slot, 0], rr_sem.at[slot, 1], to_partner)

    def resid_relay(slot):
        return remote(rt.at[slot, mate], rt.at[slot, mate], rs_sem.at[slot, 0], rr_sem.at[slot, 1], to_partner)

    def resid_received(slot):
        return remote(rt.at[slot, pl.ds(0, 2)], rt.at[slot, pl.ds(0, 2)], rs_sem.at[slot, 0], rr_sem.at[slot, 1], to_partner)

    def resid_sent(slot):
        return remote(rt.at[slot, pl.ds(0, 3)], rt.at[slot, pl.ds(0, 3)], rs_sem.at[slot, 0], rr_sem.at[slot, 1], to_partner)

    def last_rows(tile, owner, group):
        return r_out.at[tile, owner, :, targets_of(group)]

    def last_mate(slot, group, tile):
        rows = last_rows(tile, feat, group)
        return remote(rows, rows, rs_sem.at[slot, 0], rr_sem.at[slot, 0], to_mate)

    def last_partner(slot, group, tile):
        rows = last_rows(tile, feat, group)
        return remote(rows, rows, rs_sem.at[slot, 1], rr_sem.at[slot, 1], to_partner)

    def last_relay(slot, group, tile):
        rows = last_rows(tile, mate, group)
        return remote(rows, rows, rs_sem.at[slot, 2], rr_sem.at[slot, 2], to_partner)

    def grad_copy(group, index):
        return remote(gb.at[group, other * chunks + index], gr.at[group, index], gs_sem.at[group, index], gr_sem.at[group, index], to_other)

    def delta_copy(group, index, count):
        rows = pl.ds(pl.multiple_of(samp * half_feats + index * chunk, chunk), count * chunk)
        return remote(sb.at[group, rows], sb.at[group, rows], ss_sem.at[group], sr_sem.at[group], to_other)

    def coef_copy(group):
        rows = w_out.at[own_feats, targets_of(group)]
        return remote(rows, rows, wo_sem.at[group, 0], wo_sem.at[group, 1], to_other)

    def step(_, states):
        def turn_of(name):
            tile, phase, slot = states[name]
            active = (tile >= 0) & (tile < tiles) & (phase < phases)
            return active, phase >= phases - GROUPS, phase, phase & 1, tile, slot

        active_x, _, phase_x, group_x, tile_x, slot_x = turn_of("product")
        active, final, phase, group, tile, slot = turn_of("relay")
        active_s, final_s, phase_s, group_s, tile_s, slot_s = turn_of("sum")
        active_g, final_g, phase_g, group_g, tile_g, slot_g = turn_of("grad")
        turn, chunk_phase, _ = states["chunk"]
        if CHUNK_TURNS == (3, 4):
            part, index = turn & 3, 3 * lax.shift_right_logical(turn, 2) + (turn & 3)
        elif CHUNK_TURNS == (1, 2):
            part, index = turn & 1, lax.shift_right_logical(turn, 1)
        else:
            part, index = 0, turn

        @pl.when(active & jnp.logical_not(final))
        def _():
            resid_mate(slot).wait_recv()
            resid_relay(slot).start()

        @pl.when(active & final)
        def _():
            last_mate(slot, group, tile).wait_recv()
            last_relay(slot, group, tile).start()

        @pl.when((turn >= 0) & (chunk_phase < phases - GROUPS) & (part < CHUNK_TURNS[0]) & (index < chunks))
        def _():
            group = chunk_phase & 1
            grad_copy(group, index).wait()
            summed = gb[group, samp * chunks + index] + gr[group, index]
            gradient = summed.T * (1.0 / total_rows)
            rows = pl.ds(pl.multiple_of(samp * half_feats + index * chunk, chunk), chunk)
            coef = w_out[rows, targets_of(group)]
            rate = jnp.broadcast_to(eb[index], (width, chunk)).T
            delta = rate * (gradient - lb[group] * coef)
            w_out[rows, targets_of(group)] = coef + STEP_WEIGHT * delta
            sb[group, rows] = delta.astype(jnp.bfloat16)
            delta_copy(group, index, 1).start()

            @pl.when((chunk_phase == phases - GROUPS - 1) & (index == chunks - 1))
            def _():
                for each in range(GROUPS):
                    coef_copy(each).start()

        @pl.when(active_x & (tile_x == 0) & (phase_x >= GROUPS))
        def _():
            delta_copy(group_x, 0, chunks).wait()

        @pl.when(active_x & (tile_x == 0) & (phase_x == 1))
        def _():
            round_coef(1)

        @pl.when(active_x & (phase_x == 0))
        def _():
            @pl.when(tile_x < RING - AHEAD)
            def _():
                load_tile(tile_x + AHEAD, slot_x + AHEAD).start()

            @pl.when(tile_x == RING - AHEAD)
            def _():
                first_coef(1).start()

        work_g = active_g & jnp.logical_not(final_g)

        def multiply():
            delta = sb[group_x]
            product = jnp.dot(xb[slot_x], jnp.concatenate([delta, delta], axis=1), preferred_element_type=jnp.float32)
            ub[slot_x] = product[:, :width].astype(jnp.bfloat16).reshape(4, owned, width)

        def send():
            for copy in product_copies(slot_x):
                copy.start()

        def left_of(slot):
            return jnp.concatenate([rt[slot, owner] for owner in range(4)], axis=1)

        def accumulate():
            left = left_of(slot_g)
            for each in range(2 * chunks):
                share = jnp.dot(left, xb[slot_g, :, each * chunk:(each + 1) * chunk], preferred_element_type=jnp.float32)
                gb[group_g, each] = jnp.where(tile_g == 0, 0.0, gb[group_g, each]) + share

        def retire(slot, tile):
            products(slot).wait_send()

            @pl.when(phase_g * tiles + tile + RING < phases * tiles)
            def _():
                ahead = jnp.where(tile + RING >= tiles, tile + RING - tiles, tile + RING)
                load_tile(ahead, slot).start()

        slot_b = jnp.where(slot_g == 0, RING - 1, slot_g - 1)

        @pl.when(work_g & (tile_g == tiles - 1))
        def _():
            resid_received(slot_b).wait_recv()
            resid_received(slot_g).wait_recv()
            left_b, left_g = left_of(slot_b), left_of(slot_g)
            for side in (other, samp):
                for each in range(chunks):
                    feats = pl.ds(pl.multiple_of((side * chunks + each) * chunk, chunk), chunk)
                    share = jnp.dot(left_b, xb[slot_b, :, feats], preferred_element_type=jnp.float32)
                    share = share + jnp.dot(left_g, xb[slot_g, :, feats], preferred_element_type=jnp.float32)
                    gb[group_g, side * chunks + each] += share
                if side is other:
                    for each in range(chunks):
                        grad_copy(group_g, each).start()
            for slot_each, tile_each in ((slot_b, tile_g - 1), (slot_g, tile_g)):
                resid_sent(slot_each).wait_send()
                retire(slot_each, tile_each)

        single_g = work_g & (tile_g < tiles - 2)

        @pl.when(active_x & single_g)
        def _():
            load_tile(tile_x, slot_x).wait()
            resid_received(slot_g).wait_recv()
            multiply()
            accumulate()
            send()

        @pl.when(active_x & jnp.logical_not(single_g))
        def _():
            load_tile(tile_x, slot_x).wait()
            multiply()
            send()

        @pl.when(jnp.logical_not(active_x) & single_g)
        def _():
            resid_received(slot_g).wait_recv()
            accumulate()

        @pl.when(single_g)
        def _():
            resid_sent(slot_g).wait_send()
            retire(slot_g, tile_g)

        @pl.when(active_g & final_g)
        def _():
            last_partner(slot_g, group_g, tile_g).wait()
            last_relay(slot_g, group_g, tile_g).wait()
            last_mate(slot_g, group_g, tile_g).wait_send()
            retire(slot_g, tile_g)

        @pl.when(active_s & (tile_s == 0) & (phase_s == 0))
        def _():
            for copy in rest:
                copy.wait()

        @pl.when(active_s)
        def _():
            products(slot_s).wait_recv()
            summed = ub[slot_s, feat].astype(jnp.float32) + ur[slot_s, 2].astype(jnp.float32)
            summed = summed + (ur[slot_s, 0].astype(jnp.float32) + ur[slot_s, 1].astype(jnp.float32))
            weight = jnp.where(phase_s < GROUPS, 1.0, STEP_WEIGHT)
            resid = r_out[tile_s, feat, :, targets_of(group_s)] - weight * summed
            r_out[tile_s, feat, :, targets_of(group_s)] = resid

            @pl.when(jnp.logical_not(final_s))
            def _():
                rt[slot_s, feat] = resid.astype(jnp.bfloat16).T
                resid_mate(slot_s).start()
                resid_partner(slot_s).start()

            @pl.when(final_s)
            def _():
                last_mate(slot_s, group_s, tile_s).start()
                last_partner(slot_s, group_s, tile_s).start()

        following = {}
        for name, (tile, phase, slot) in states.items():
            within = (tile >= 0) & (tile < tiles)
            slot = jnp.where(within, slot + 1, slot)
            wrap = tile == jnp.where(phase == phases - GROUPS, short - 1, steps - 1)
            following[name] = (
                jnp.where(wrap, 0, tile + 1),
                jnp.where(wrap, phase + 1, phase),
                jnp.where(slot == RING, 0, slot),
            )
        return following

    zero = jnp.int32(0)
    lags = {"product": 0, "sum": LAG_SUM, "relay": LAG_RELAY, "grad": LAG_GRAD, "chunk": grad_end + FIRST_CHUNK}
    start = {name: (jnp.int32(-lag), zero, zero) for name, lag in lags.items()}
    lax.fori_loop(0, (phases - 2) * steps + short + tiles + LAG_GRAD, step, start)
    for group in range(GROUPS):
        coef_copy(group).wait()


def sweeps(design, targets, coef_init, step_sizes, ridge_weights):
    rows, feats = design.shape
    width = targets.shape[1] // GROUPS
    owned = 128
    tiles = rows // (4 * owned)
    chunks = 8
    chunk = feats // (2 * chunks)
    dma = pltpu.SemaphoreType.DMA
    f32, bf16 = jnp.float32, jnp.bfloat16
    scratch = [
        pltpu.VMEM((RING, 4 * owned, feats), bf16),
        pltpu.VMEM((GROUPS, feats, width), bf16),
        pltpu.VMEM((GROUPS, 2 * chunks, width, chunk), f32),
        pltpu.VMEM((GROUPS, chunks, width, chunk), f32),
        pltpu.VMEM((chunks, 1, chunk), f32),
        pltpu.VMEM((GROUPS, 1, width), f32),
        pltpu.VMEM((RING, 4, width, owned), bf16),
        pltpu.VMEM((RING, 4, owned, width), bf16),
        pltpu.VMEM((RING, 3, owned, width), bf16),
        dma((RING,)),
        dma((GROUPS + 3,)),
        dma((RING,)),
        dma((RING,)),
        dma((RING, 3)),
        dma((RING, 3)),
        dma((GROUPS, chunks)),
        dma((GROUPS, chunks)),
        dma((GROUPS,)),
        dma((GROUPS,)),
        dma((GROUPS, 2)),
    ]
    tiled = (tiles, 4, owned, targets.shape[1])
    coef, resid = pl.pallas_call(
        kernel,
        out_shape=(pltpu.VMEM(coef_init.shape, f32), pltpu.VMEM(tiled, f32)),
        in_specs=[pl.BlockSpec(memory_space=pl.ANY)] * 5,
        out_specs=[pl.BlockSpec(memory_space=pltpu.VMEM)] * 2,
        scratch_shapes=scratch,
        compiler_params=pltpu.CompilerParams(collective_id=0, has_side_effects=True, vmem_limit_bytes=519 * 2**20 // 10),
    )(
        design,
        targets.reshape(tiled),
        coef_init,
        step_sizes.reshape(2 * chunks, 1, chunk),
        ridge_weights.reshape(GROUPS, 1, width),
    )
    return coef, resid.reshape(targets.shape)


def solution(mesh):
    design_spec = P(("problem", "samp"), "feat")
    rows_spec = P(("problem", "samp"), None)
    coef_spec = P(("problem", "feat"), None)
    step_spec = P(("problem", "feat"))
    ridge_spec = P("problem")
    return jax.shard_map(sweeps, mesh=mesh, in_specs=(design_spec, rows_spec, coef_spec, step_spec, ridge_spec), out_specs=(coef_spec, rows_spec), check_vma=False)
```

```python
import functools

import jax
import jax.numpy as jnp
from jax import lax
from jax.experimental import pallas as pl
from jax.experimental.pallas import tpu as pltpu
from jax.sharding import PartitionSpec as P

SWEEPS = 4
STEP_WEIGHT = 0.5
MESH = pl.DeviceIdType.MESH

RING = 10
AHEAD = 2
LAG_SUM = 3
LAG_RELAY = 7
LAG_GRAD = 8
EXTRA = 6
EXTRA_LAST = 2
FIRST_CHUNK = 7
CHUNK_TURNS = (3, 4)
PIECES = 4
GROUPS = 2


def kernel(x_hbm, y_hbm, w0_hbm, eta_hbm, lam_hbm, w_out, r_out,
           xb, sb, gb, gr, eb, lb, rt, ub, ur,
           x_sem, in_sem, us_sem, ur_sem, rs_sem, rr_sem, gs_sem, gr_sem, ss_sem, sr_sem, wo_sem):
    problem, samp, feat = lax.axis_index("problem"), lax.axis_index("samp"), lax.axis_index("feat")
    partner = feat + 1 - 2 * lax.rem(feat, 2)
    mate = lax.rem(feat + 2, 4)
    cross = lax.rem(partner + 2, 4)
    to_partner, to_mate, to_cross = (problem, samp, partner), (problem, samp, mate), (problem, samp, cross)
    other = 1 - samp
    to_other = (problem, other, feat)

    owned = r_out.shape[2]
    tile_rows = 4 * owned
    tiles = r_out.shape[0]
    width = gb.shape[2]
    chunks = gr.shape[1]
    chunk = gb.shape[3]
    half_feats = chunks * chunk
    phases = GROUPS * (SWEEPS + 1)
    steps, short = tiles + EXTRA, tiles + EXTRA_LAST
    grad_end = tiles - 1 + LAG_GRAD
    total_rows = 2 * tiles * tile_rows

    def remote(src, dst, send, recv, device):
        return pltpu.make_async_remote_copy(src_ref=src, dst_ref=dst, send_sem=send, recv_sem=recv, device_id=device, device_id_type=MESH)

    barrier = pltpu.get_barrier_semaphore()
    for device in (to_partner, to_mate, to_cross, to_other):
        pl.semaphore_signal(barrier, inc=1, device_id=device, device_id_type=MESH)

    def load_tile(tile, slot):
        rows = pl.ds(pl.multiple_of(tile * tile_rows, tile_rows), tile_rows)
        return pltpu.make_async_copy(x_hbm.at[rows], xb.at[slot], x_sem.at[slot])

    own_feats = pl.ds(pl.multiple_of(samp * half_feats, half_feats), half_feats)
    other_feats = pl.ds(pl.multiple_of(other * half_feats, half_feats), half_feats)

    def targets_of(group):
        return pl.ds(pl.multiple_of(group * width, width), width)

    def first_coef(group):
        return pltpu.make_async_copy(w0_hbm.at[:, targets_of(group)], w_out.at[:, targets_of(group)], in_sem.at[group])

    def round_coef(group):
        first_coef(group).wait()
        for each in range(2 * chunks):
            rows = pl.ds(each * chunk, chunk)
            sb[group, rows] = w_out[rows, group * width:(group + 1) * width].astype(jnp.bfloat16)

    rest = [
        pltpu.make_async_copy(y_hbm.at[:, feat], r_out.at[:, feat], in_sem.at[GROUPS]),
        pltpu.make_async_copy(eta_hbm.at[pl.ds(samp * chunks, chunks)], eb, in_sem.at[GROUPS + 1]),
        pltpu.make_async_copy(lam_hbm, lb, in_sem.at[GROUPS + 2]),
    ]
    first_coef(0).start()
    load_tile(0, 0).start()
    for slot in range(1, AHEAD):
        load_tile(slot, slot).start()
    round_coef(0)
    for copy in rest:
        copy.start()
    pl.semaphore_wait(barrier, 4)

    def product_copies(slot):
        return [
            remote(ub.at[slot, owner], ur.at[slot, rel], us_sem.at[slot], ur_sem.at[slot], device)
            for rel, (owner, device) in enumerate(((mate, to_mate), (cross, to_cross), (partner, to_partner)))
        ]

    def products(slot):
        return remote(ur.at[slot], ur.at[slot], us_sem.at[slot], ur_sem.at[slot], to_partner)

    def resid_mate(slot):
        return remote(rt.at[slot, feat], rt.at[slot, feat], rs_sem.at[slot, 0], rr_sem.at[slot, 0], to_mate)

    def resid_partner(slot):
        return remote(rt.at[slot, feat], rt.at[slot, feat], rs_sem.at[slot, 0], rr_sem.at[slot, 1], to_partner)

    def resid_relay(slot):
        return remote(rt.at[slot, mate], rt.at[slot, mate], rs_sem.at[slot, 0], rr_sem.at[slot, 1], to_partner)

    def resid_received(slot):
        return remote(rt.at[slot, pl.ds(0, 2)], rt.at[slot, pl.ds(0, 2)], rs_sem.at[slot, 0], rr_sem.at[slot, 1], to_partner)

    def resid_sent(slot):
        return remote(rt.at[slot, pl.ds(0, 3)], rt.at[slot, pl.ds(0, 3)], rs_sem.at[slot, 0], rr_sem.at[slot, 1], to_partner)

    def last_rows(tile, owner, group):
        return r_out.at[tile, owner, :, targets_of(group)]

    def last_mate(slot, group, tile):
        rows = last_rows(tile, feat, group)
        return remote(rows, rows, rs_sem.at[slot, 0], rr_sem.at[slot, 0], to_mate)

    def last_partner(slot, group, tile):
        rows = last_rows(tile, feat, group)
        return remote(rows, rows, rs_sem.at[slot, 1], rr_sem.at[slot, 1], to_partner)

    def last_relay(slot, group, tile):
        rows = last_rows(tile, mate, group)
        return remote(rows, rows, rs_sem.at[slot, 2], rr_sem.at[slot, 2], to_partner)

    def grad_copy(group, index):
        return remote(gb.at[group, other * chunks + index], gr.at[group, index], gs_sem.at[group, index], gr_sem.at[group, index], to_other)

    def delta_copy(group, index, count):
        rows = pl.ds(pl.multiple_of(samp * half_feats + index * chunk, chunk), count * chunk)
        return remote(sb.at[group, rows], sb.at[group, rows], ss_sem.at[group], sr_sem.at[group], to_other)

    def coef_copy(group):
        rows = w_out.at[own_feats, targets_of(group)]
        return remote(rows, rows, wo_sem.at[group, 0], wo_sem.at[group, 1], to_other)

    def step(_, states):
        def turn_of(name):
            tile, phase, slot = states[name]
            active = (tile >= 0) & (tile < tiles) & (phase < phases)
            return active, phase >= phases - GROUPS, phase, phase & 1, tile, slot

        active_x, _, phase_x, group_x, tile_x, slot_x = turn_of("product")
        active, final, phase, group, tile, slot = turn_of("relay")
        active_s, final_s, phase_s, group_s, tile_s, slot_s = turn_of("sum")
        active_g, final_g, phase_g, group_g, tile_g, slot_g = turn_of("grad")
        turn, chunk_phase, _ = states["chunk"]
        if CHUNK_TURNS == (3, 4):
            part, index = turn & 3, 3 * lax.shift_right_logical(turn, 2) + (turn & 3)
        elif CHUNK_TURNS == (1, 2):
            part, index = turn & 1, lax.shift_right_logical(turn, 1)
        else:
            part, index = 0, turn

        @pl.when(active & jnp.logical_not(final))
        def _():
            resid_mate(slot).wait_recv()
            resid_relay(slot).start()

        @pl.when(active & final)
        def _():
            last_mate(slot, group, tile).wait_recv()
            last_relay(slot, group, tile).start()

        @pl.when((turn >= 0) & (chunk_phase < phases - GROUPS) & (part < CHUNK_TURNS[0]) & (index < chunks))
        def _():
            group = chunk_phase & 1
            grad_copy(group, index).wait()
            summed = gb[group, samp * chunks + index] + gr[group, index]
            gradient = summed.T * (1.0 / total_rows)
            rows = pl.ds(pl.multiple_of(samp * half_feats + index * chunk, chunk), chunk)
            coef = w_out[rows, targets_of(group)]
            rate = jnp.broadcast_to(eb[index], (width, chunk)).T
            delta = rate * (gradient - lb[group] * coef)
            w_out[rows, targets_of(group)] = coef + STEP_WEIGHT * delta
            sb[group, rows] = delta.astype(jnp.bfloat16)
            delta_copy(group, index, 1).start()

            @pl.when((chunk_phase == phases - GROUPS - 1) & (index == chunks - 1))
            def _():
                for each in range(GROUPS):
                    coef_copy(each).start()

        @pl.when(active_x & (tile_x == 0) & (phase_x >= GROUPS))
        def _():
            delta_copy(group_x, 0, chunks).wait()

        @pl.when(active_x & (tile_x == 0) & (phase_x == 1))
        def _():
            round_coef(1)

        @pl.when(active_x & (phase_x == 0))
        def _():
            @pl.when(tile_x < RING - AHEAD)
            def _():
                load_tile(tile_x + AHEAD, slot_x + AHEAD).start()

            @pl.when(tile_x == RING - AHEAD)
            def _():
                first_coef(1).start()

        work_g = active_g & jnp.logical_not(final_g)

        def multiply():
            delta = sb[group_x]
            product = jnp.dot(xb[slot_x], jnp.concatenate([delta, delta], axis=1), preferred_element_type=jnp.float32)
            ub[slot_x] = product[:, :width].astype(jnp.bfloat16).reshape(4, owned, width)

        def send():
            for copy in product_copies(slot_x):
                copy.start()

        def accumulate():
            left = jnp.concatenate([rt[slot_g, owner] for owner in range(4)], axis=1)
            for each in range(2 * chunks):
                share = jnp.dot(left, xb[slot_g, :, each * chunk:(each + 1) * chunk], preferred_element_type=jnp.float32)
                gb[group_g, each] = jnp.where(tile_g == 0, 0.0, gb[group_g, each]) + share

        @pl.when(active_x & work_g)
        def _():
            load_tile(tile_x, slot_x).wait()
            resid_received(slot_g).wait_recv()
            multiply()
            accumulate()
            send()

        @pl.when(active_x & jnp.logical_not(work_g))
        def _():
            load_tile(tile_x, slot_x).wait()
            multiply()
            send()

        @pl.when(jnp.logical_not(active_x) & work_g)
        def _():
            resid_received(slot_g).wait_recv()
            accumulate()

        @pl.when(work_g)
        def _():
            @pl.when(tile_g == tiles - 1)
            def _():
                for each in range(chunks):
                    grad_copy(group_g, each).start()

            resid_sent(slot_g).wait_send()

        @pl.when(active_g & final_g)
        def _():
            last_partner(slot_g, group_g, tile_g).wait()
            last_relay(slot_g, group_g, tile_g).wait()
            last_mate(slot_g, group_g, tile_g).wait_send()

        @pl.when(active_g)
        def _():
            products(slot_g).wait_send()

            @pl.when(phase_g * tiles + tile_g + RING < phases * tiles)
            def _():
                ahead = jnp.where(tile_g + RING >= tiles, tile_g + RING - tiles, tile_g + RING)
                load_tile(ahead, slot_g).start()

        @pl.when(active_s & (tile_s == 0) & (phase_s == 0))
        def _():
            for copy in rest:
                copy.wait()

        @pl.when(active_s)
        def _():
            products(slot_s).wait_recv()
            summed = ub[slot_s, feat].astype(jnp.float32) + ur[slot_s, 2].astype(jnp.float32)
            summed = summed + (ur[slot_s, 0].astype(jnp.float32) + ur[slot_s, 1].astype(jnp.float32))
            weight = jnp.where(phase_s < GROUPS, 1.0, STEP_WEIGHT)
            resid = r_out[tile_s, feat, :, targets_of(group_s)] - weight * summed
            r_out[tile_s, feat, :, targets_of(group_s)] = resid

            @pl.when(jnp.logical_not(final_s))
            def _():
                rt[slot_s, feat] = resid.astype(jnp.bfloat16).T
                resid_mate(slot_s).start()
                resid_partner(slot_s).start()

            @pl.when(final_s)
            def _():
                last_mate(slot_s, group_s, tile_s).start()
                last_partner(slot_s, group_s, tile_s).start()

        following = {}
        for name, (tile, phase, slot) in states.items():
            within = (tile >= 0) & (tile < tiles)
            slot = jnp.where(within, slot + 1, slot)
            wrap = tile == jnp.where(phase == phases - GROUPS, short - 1, steps - 1)
            following[name] = (
                jnp.where(wrap, 0, tile + 1),
                jnp.where(wrap, phase + 1, phase),
                jnp.where(slot == RING, 0, slot),
            )
        return following

    zero = jnp.int32(0)
    lags = {"product": 0, "sum": LAG_SUM, "relay": LAG_RELAY, "grad": LAG_GRAD, "chunk": grad_end + FIRST_CHUNK}
    start = {name: (jnp.int32(-lag), zero, zero) for name, lag in lags.items()}
    lax.fori_loop(0, (phases - 2) * steps + short + tiles + LAG_GRAD, step, start)
    for group in range(GROUPS):
        coef_copy(group).wait()


def write_out(coef, resid, coef_out, resid_out, sem):
    copies = []
    for source, target in ((coef, coef_out), (resid, resid_out)):
        rows = source.shape[0] // PIECES
        for piece in range(PIECES):
            part = pl.ds(piece * rows, rows)
            copies.append(pltpu.make_async_copy(source.at[part], target.at[part], sem.at[len(copies)]))
    for copy in copies:
        copy.start()
    for copy in copies:
        copy.wait()


def sweeps(design, targets, coef_init, step_sizes, ridge_weights):
    rows, feats = design.shape
    width = targets.shape[1] // GROUPS
    owned = 128
    tiles = rows // (4 * owned)
    chunks = 8
    chunk = feats // (2 * chunks)
    dma = pltpu.SemaphoreType.DMA
    f32, bf16 = jnp.float32, jnp.bfloat16
    scratch = [
        pltpu.VMEM((RING, 4 * owned, feats), bf16),
        pltpu.VMEM((GROUPS, feats, width), bf16),
        pltpu.VMEM((GROUPS, 2 * chunks, width, chunk), f32),
        pltpu.VMEM((GROUPS, chunks, width, chunk), f32),
        pltpu.VMEM((chunks, 1, chunk), f32),
        pltpu.VMEM((GROUPS, 1, width), f32),
        pltpu.VMEM((RING, 4, width, owned), bf16),
        pltpu.VMEM((RING, 4, owned, width), bf16),
        pltpu.VMEM((RING, 3, owned, width), bf16),
        dma((RING,)),
        dma((GROUPS + 3,)),
        dma((RING,)),
        dma((RING,)),
        dma((RING, 3)),
        dma((RING, 3)),
        dma((GROUPS, chunks)),
        dma((GROUPS, chunks)),
        dma((GROUPS,)),
        dma((GROUPS,)),
        dma((GROUPS, 2)),
    ]
    tiled = (tiles, 4, owned, targets.shape[1])
    coef, resid = pl.pallas_call(
        kernel,
        out_shape=(pltpu.VMEM(coef_init.shape, f32), pltpu.VMEM(tiled, f32)),
        in_specs=[pl.BlockSpec(memory_space=pl.ANY)] * 5,
        out_specs=[pl.BlockSpec(memory_space=pltpu.VMEM)] * 2,
        scratch_shapes=scratch,
        compiler_params=pltpu.CompilerParams(collective_id=0, has_side_effects=True, vmem_limit_bytes=519 * 2**20 // 10),
    )(
        design,
        targets.reshape(tiled),
        coef_init,
        step_sizes.reshape(2 * chunks, 1, chunk),
        ridge_weights.reshape(GROUPS, 1, width),
    )
    coef, resid = pl.pallas_call(
        write_out,
        out_shape=(jax.ShapeDtypeStruct(coef.shape, f32), jax.ShapeDtypeStruct(tiled, f32)),
        in_specs=[pl.BlockSpec(memory_space=pl.ANY)] * 2,
        out_specs=[pl.BlockSpec(memory_space=pl.ANY)] * 2,
        scratch_shapes=[dma((2 * PIECES,))],
        compiler_params=pltpu.CompilerParams(vmem_limit_bytes=2**20),
    )(pltpu.with_memory_space_constraint(coef, pltpu.VMEM), pltpu.with_memory_space_constraint(resid, pltpu.VMEM))
    return coef, resid.reshape(targets.shape)


def solution(mesh):
    design_spec = P(("problem", "samp"), "feat")
    rows_spec = P(("problem", "samp"), None)
    coef_spec = P(("problem", "feat"), None)
    step_spec = P(("problem", "feat"))
    ridge_spec = P("problem")
    return jax.shard_map(sweeps, mesh=mesh, in_specs=(design_spec, rows_spec, coef_spec, step_spec, ridge_spec), out_specs=(coef_spec, rows_spec), check_vma=False)
```

```python
import functools

import jax
import jax.numpy as jnp
from jax import lax
from jax.experimental import pallas as pl
from jax.experimental.pallas import tpu as pltpu
from jax.sharding import PartitionSpec as P

SWEEPS = 4
STEP_WEIGHT = 0.5
MESH = pl.DeviceIdType.MESH

RING = 10
AHEAD = 2
LAG_SUM = 3
LAG_RELAY = 7
LAG_GRAD = 8
EXTRA = 7
EXTRA_LAST = 2
FIRST_CHUNK = 6
CHUNK_TURNS = (3, 4)
PIECES = 4
GROUPS = 2


def kernel(x_hbm, y_hbm, w0_hbm, eta_hbm, lam_hbm, w_out, r_out,
           xb, sb, gb, gr, eb, lb, rt, ub, ur,
           x_sem, in_sem, us_sem, ur_sem, rs_sem, rr_sem, gs_sem, gr_sem, ss_sem, sr_sem, wo_sem):
    problem, samp, feat = lax.axis_index("problem"), lax.axis_index("samp"), lax.axis_index("feat")
    partner = feat + 1 - 2 * lax.rem(feat, 2)
    mate = lax.rem(feat + 2, 4)
    cross = lax.rem(partner + 2, 4)
    to_partner, to_mate, to_cross = (problem, samp, partner), (problem, samp, mate), (problem, samp, cross)
    other = 1 - samp
    to_other = (problem, other, feat)

    owned = r_out.shape[2]
    tile_rows = 4 * owned
    tiles = r_out.shape[0]
    width = gb.shape[2]
    chunks = gr.shape[1]
    chunk = gb.shape[3]
    half_feats = chunks * chunk
    phases = GROUPS * (SWEEPS + 1)
    steps, short = tiles + EXTRA, tiles + EXTRA_LAST
    grad_end = tiles - 1 + LAG_GRAD
    total_rows = 2 * tiles * tile_rows

    def remote(src, dst, send, recv, device):
        return pltpu.make_async_remote_copy(src_ref=src, dst_ref=dst, send_sem=send, recv_sem=recv, device_id=device, device_id_type=MESH)

    barrier = pltpu.get_barrier_semaphore()
    for device in (to_partner, to_mate, to_cross, to_other):
        pl.semaphore_signal(barrier, inc=1, device_id=device, device_id_type=MESH)

    def load_tile(tile, slot):
        rows = pl.ds(pl.multiple_of(tile * tile_rows, tile_rows), tile_rows)
        return pltpu.make_async_copy(x_hbm.at[rows], xb.at[slot], x_sem.at[slot])

    own_feats = pl.ds(pl.multiple_of(samp * half_feats, half_feats), half_feats)
    other_feats = pl.ds(pl.multiple_of(other * half_feats, half_feats), half_feats)

    def targets_of(group):
        return pl.ds(pl.multiple_of(group * width, width), width)

    def first_coef(group):
        return pltpu.make_async_copy(w0_hbm.at[:, targets_of(group)], w_out.at[:, targets_of(group)], in_sem.at[group])

    def round_coef(group):
        first_coef(group).wait()
        for each in range(2 * chunks):
            rows = pl.ds(each * chunk, chunk)
            sb[group, rows] = w_out[rows, group * width:(group + 1) * width].astype(jnp.bfloat16)

    rest = [
        pltpu.make_async_copy(y_hbm.at[:, feat], r_out.at[:, feat], in_sem.at[GROUPS]),
        pltpu.make_async_copy(eta_hbm.at[pl.ds(samp * chunks, chunks)], eb, in_sem.at[GROUPS + 1]),
        pltpu.make_async_copy(lam_hbm, lb, in_sem.at[GROUPS + 2]),
    ]
    first_coef(0).start()
    load_tile(0, 0).start()
    for slot in range(1, AHEAD):
        load_tile(slot, slot).start()
    round_coef(0)
    for copy in rest:
        copy.start()
    pl.semaphore_wait(barrier, 4)

    def product_copies(slot):
        return [
            remote(ub.at[slot, owner], ur.at[slot, rel], us_sem.at[slot], ur_sem.at[slot], device)
            for rel, (owner, device) in enumerate(((mate, to_mate), (cross, to_cross), (partner, to_partner)))
        ]

    def products(slot):
        return remote(ur.at[slot], ur.at[slot], us_sem.at[slot], ur_sem.at[slot], to_partner)

    def resid_mate(slot):
        return remote(rt.at[slot, feat], rt.at[slot, feat], rs_sem.at[slot, 0], rr_sem.at[slot, 0], to_mate)

    def resid_partner(slot):
        return remote(rt.at[slot, feat], rt.at[slot, feat], rs_sem.at[slot, 0], rr_sem.at[slot, 1], to_partner)

    def resid_relay(slot):
        return remote(rt.at[slot, mate], rt.at[slot, mate], rs_sem.at[slot, 0], rr_sem.at[slot, 1], to_partner)

    def resid_received(slot):
        return remote(rt.at[slot, pl.ds(0, 2)], rt.at[slot, pl.ds(0, 2)], rs_sem.at[slot, 0], rr_sem.at[slot, 1], to_partner)

    def resid_sent(slot):
        return remote(rt.at[slot, pl.ds(0, 3)], rt.at[slot, pl.ds(0, 3)], rs_sem.at[slot, 0], rr_sem.at[slot, 1], to_partner)

    def last_rows(tile, owner, group):
        return r_out.at[tile, owner, :, targets_of(group)]

    def last_mate(slot, group, tile):
        rows = last_rows(tile, feat, group)
        return remote(rows, rows, rs_sem.at[slot, 0], rr_sem.at[slot, 0], to_mate)

    def last_partner(slot, group, tile):
        rows = last_rows(tile, feat, group)
        return remote(rows, rows, rs_sem.at[slot, 1], rr_sem.at[slot, 1], to_partner)

    def last_relay(slot, group, tile):
        rows = last_rows(tile, mate, group)
        return remote(rows, rows, rs_sem.at[slot, 2], rr_sem.at[slot, 2], to_partner)

    def grad_copy(group, index):
        return remote(gb.at[group, other * chunks + index], gr.at[group, index], gs_sem.at[group, index], gr_sem.at[group, index], to_other)

    def delta_copy(group, index, count):
        rows = pl.ds(pl.multiple_of(samp * half_feats + index * chunk, chunk), count * chunk)
        return remote(sb.at[group, rows], sb.at[group, rows], ss_sem.at[group], sr_sem.at[group], to_other)

    def coef_copy(group):
        rows = w_out.at[own_feats, targets_of(group)]
        return remote(rows, rows, wo_sem.at[group, 0], wo_sem.at[group, 1], to_other)

    def step(_, states):
        def turn_of(name):
            tile, phase, slot = states[name]
            active = (tile >= 0) & (tile < tiles) & (phase < phases)
            return active, phase >= phases - GROUPS, phase, phase & 1, tile, slot

        active_x, _, phase_x, group_x, tile_x, slot_x = turn_of("product")
        active, final, phase, group, tile, slot = turn_of("relay")
        active_s, final_s, phase_s, group_s, tile_s, slot_s = turn_of("sum")
        active_g, final_g, phase_g, group_g, tile_g, slot_g = turn_of("grad")
        turn, chunk_phase, _ = states["chunk"]
        if CHUNK_TURNS == (3, 4):
            part, index = turn & 3, 3 * lax.shift_right_logical(turn, 2) + (turn & 3)
        elif CHUNK_TURNS == (1, 2):
            part, index = turn & 1, lax.shift_right_logical(turn, 1)
        else:
            part, index = 0, turn

        @pl.when(active & jnp.logical_not(final))
        def _():
            resid_mate(slot).wait_recv()
            resid_relay(slot).start()

        @pl.when(active & final)
        def _():
            last_mate(slot, group, tile).wait_recv()
            last_relay(slot, group, tile).start()

        @pl.when((turn >= 0) & (chunk_phase < phases - GROUPS) & (part < CHUNK_TURNS[0]) & (index < chunks))
        def _():
            group = chunk_phase & 1
            grad_copy(group, index).wait()
            summed = gb[group, samp * chunks + index] + gr[group, index]
            gradient = summed.T * (1.0 / total_rows)
            rows = pl.ds(pl.multiple_of(samp * half_feats + index * chunk, chunk), chunk)
            coef = w_out[rows, targets_of(group)]
            rate = jnp.broadcast_to(eb[index], (width, chunk)).T
            delta = rate * (gradient - lb[group] * coef)
            w_out[rows, targets_of(group)] = coef + STEP_WEIGHT * delta
            sb[group, rows] = delta.astype(jnp.bfloat16)
            delta_copy(group, index, 1).start()

            @pl.when((chunk_phase == phases - GROUPS - 1) & (index == chunks - 1))
            def _():
                for each in range(GROUPS):
                    coef_copy(each).start()

        @pl.when(active_x & (tile_x == 0) & (phase_x >= GROUPS))
        def _():
            delta_copy(group_x, 0, chunks).wait()

        @pl.when(active_x & (tile_x == 0) & (phase_x == 1))
        def _():
            round_coef(1)

        @pl.when(active_x & (phase_x == 0))
        def _():
            @pl.when(tile_x < RING - AHEAD)
            def _():
                load_tile(tile_x + AHEAD, slot_x + AHEAD).start()

            @pl.when(tile_x == RING - AHEAD)
            def _():
                first_coef(1).start()

        work_g = active_g & jnp.logical_not(final_g)

        def multiply():
            delta = sb[group_x]
            product = jnp.dot(xb[slot_x], jnp.concatenate([delta, delta], axis=1), preferred_element_type=jnp.float32)
            ub[slot_x] = product[:, :width].astype(jnp.bfloat16).reshape(4, owned, width)

        def send():
            for copy in product_copies(slot_x):
                copy.start()

        def accumulate():
            left = jnp.concatenate([rt[slot_g, owner] for owner in range(4)], axis=1)
            for each in range(2 * chunks):
                share = jnp.dot(left, xb[slot_g, :, each * chunk:(each + 1) * chunk], preferred_element_type=jnp.float32)
                gb[group_g, each] = jnp.where(tile_g == 0, 0.0, gb[group_g, each]) + share

        @pl.when(active_x & work_g)
        def _():
            load_tile(tile_x, slot_x).wait()
            resid_received(slot_g).wait_recv()
            multiply()
            accumulate()
            send()

        @pl.when(active_x & jnp.logical_not(work_g))
        def _():
            load_tile(tile_x, slot_x).wait()
            multiply()
            send()

        @pl.when(jnp.logical_not(active_x) & work_g)
        def _():
            resid_received(slot_g).wait_recv()
            accumulate()

        @pl.when(work_g)
        def _():
            @pl.when(tile_g == tiles - 1)
            def _():
                for each in range(chunks):
                    grad_copy(group_g, each).start()

            resid_sent(slot_g).wait_send()

        @pl.when(active_g & final_g)
        def _():
            last_partner(slot_g, group_g, tile_g).wait()
            last_relay(slot_g, group_g, tile_g).wait()
            last_mate(slot_g, group_g, tile_g).wait_send()

        @pl.when(active_g)
        def _():
            products(slot_g).wait_send()

            @pl.when(phase_g * tiles + tile_g + RING < phases * tiles)
            def _():
                ahead = jnp.where(tile_g + RING >= tiles, tile_g + RING - tiles, tile_g + RING)
                load_tile(ahead, slot_g).start()

        @pl.when(active_s & (tile_s == 0) & (phase_s == 0))
        def _():
            for copy in rest:
                copy.wait()

        @pl.when(active_s)
        def _():
            products(slot_s).wait_recv()
            summed = ub[slot_s, feat].astype(jnp.float32) + ur[slot_s, 2].astype(jnp.float32)
            summed = summed + (ur[slot_s, 0].astype(jnp.float32) + ur[slot_s, 1].astype(jnp.float32))
            weight = jnp.where(phase_s < GROUPS, 1.0, STEP_WEIGHT)
            resid = r_out[tile_s, feat, :, targets_of(group_s)] - weight * summed
            r_out[tile_s, feat, :, targets_of(group_s)] = resid

            @pl.when(jnp.logical_not(final_s))
            def _():
                rt[slot_s, feat] = resid.astype(jnp.bfloat16).T
                resid_mate(slot_s).start()
                resid_partner(slot_s).start()

            @pl.when(final_s)
            def _():
                last_mate(slot_s, group_s, tile_s).start()
                last_partner(slot_s, group_s, tile_s).start()

        following = {}
        for name, (tile, phase, slot) in states.items():
            within = (tile >= 0) & (tile < tiles)
            slot = jnp.where(within, slot + 1, slot)
            wrap = tile == jnp.where(phase == phases - GROUPS, short - 1, steps - 1)
            following[name] = (
                jnp.where(wrap, 0, tile + 1),
                jnp.where(wrap, phase + 1, phase),
                jnp.where(slot == RING, 0, slot),
            )
        return following

    zero = jnp.int32(0)
    lags = {"product": 0, "sum": LAG_SUM, "relay": LAG_RELAY, "grad": LAG_GRAD, "chunk": grad_end + FIRST_CHUNK}
    start = {name: (jnp.int32(-lag), zero, zero) for name, lag in lags.items()}
    lax.fori_loop(0, (phases - 2) * steps + short + tiles + LAG_GRAD, step, start)
    for group in range(GROUPS):
        coef_copy(group).wait()


def write_out(coef, resid, coef_out, resid_out, sem):
    copies = []
    for source, target in ((coef, coef_out), (resid, resid_out)):
        rows = source.shape[0] // PIECES
        for piece in range(PIECES):
            part = pl.ds(piece * rows, rows)
            copies.append(pltpu.make_async_copy(source.at[part], target.at[part], sem.at[len(copies)]))
    for copy in copies:
        copy.start()
    for copy in copies:
        copy.wait()


def sweeps(design, targets, coef_init, step_sizes, ridge_weights):
    rows, feats = design.shape
    width = targets.shape[1] // GROUPS
    owned = 128
    tiles = rows // (4 * owned)
    chunks = 8
    chunk = feats // (2 * chunks)
    dma = pltpu.SemaphoreType.DMA
    f32, bf16 = jnp.float32, jnp.bfloat16
    scratch = [
        pltpu.VMEM((RING, 4 * owned, feats), bf16),
        pltpu.VMEM((GROUPS, feats, width), bf16),
        pltpu.VMEM((GROUPS, 2 * chunks, width, chunk), f32),
        pltpu.VMEM((GROUPS, chunks, width, chunk), f32),
        pltpu.VMEM((chunks, 1, chunk), f32),
        pltpu.VMEM((GROUPS, 1, width), f32),
        pltpu.VMEM((RING, 4, width, owned), bf16),
        pltpu.VMEM((RING, 4, owned, width), bf16),
        pltpu.VMEM((RING, 3, owned, width), bf16),
        dma((RING,)),
        dma((GROUPS + 3,)),
        dma((RING,)),
        dma((RING,)),
        dma((RING, 3)),
        dma((RING, 3)),
        dma((GROUPS, chunks)),
        dma((GROUPS, chunks)),
        dma((GROUPS,)),
        dma((GROUPS,)),
        dma((GROUPS, 2)),
    ]
    tiled = (tiles, 4, owned, targets.shape[1])
    coef, resid = pl.pallas_call(
        kernel,
        out_shape=(pltpu.VMEM(coef_init.shape, f32), pltpu.VMEM(tiled, f32)),
        in_specs=[pl.BlockSpec(memory_space=pl.ANY)] * 5,
        out_specs=[pl.BlockSpec(memory_space=pltpu.VMEM)] * 2,
        scratch_shapes=scratch,
        compiler_params=pltpu.CompilerParams(collective_id=0, has_side_effects=True, vmem_limit_bytes=519 * 2**20 // 10),
    )(
        design,
        targets.reshape(tiled),
        coef_init,
        step_sizes.reshape(2 * chunks, 1, chunk),
        ridge_weights.reshape(GROUPS, 1, width),
    )
    coef, resid = pl.pallas_call(
        write_out,
        out_shape=(jax.ShapeDtypeStruct(coef.shape, f32), jax.ShapeDtypeStruct(tiled, f32)),
        in_specs=[pl.BlockSpec(memory_space=pl.ANY)] * 2,
        out_specs=[pl.BlockSpec(memory_space=pl.ANY)] * 2,
        scratch_shapes=[dma((2 * PIECES,))],
        compiler_params=pltpu.CompilerParams(vmem_limit_bytes=2**20),
    )(pltpu.with_memory_space_constraint(coef, pltpu.VMEM), pltpu.with_memory_space_constraint(resid, pltpu.VMEM))
    return coef, resid.reshape(targets.shape)


def solution(mesh):
    design_spec = P(("problem", "samp"), "feat")
    rows_spec = P(("problem", "samp"), None)
    coef_spec = P(("problem", "feat"), None)
    step_spec = P(("problem", "feat"))
    ridge_spec = P("problem")
    return jax.shard_map(sweeps, mesh=mesh, in_specs=(design_spec, rows_spec, coef_spec, step_spec, ridge_spec), out_specs=(coef_spec, rows_spec), check_vma=False)
```
